32 devices in a mesh: curve: 16 (over z, y, core), tm: 2 (over x).
Axes of the slice: x: 2, y: 2, z: 4, core: 2. Of those that a mesh axis runs over, the one named last changes fastest.
Arguments:
- samples: float32 [4096, 65536], P('curve', 'tm'), may hold values from -30 to 30
- smoothing: float32 [4096], P('curve'), may hold values from 0.5 to 20
- test_matrix: float32 [4096, 64], P('tm'), may hold values from -0.75 to 0.75
- sketch_prev: float32 [4096, 64], P('tm', 'curve'), may hold values from -1.2 to 1.2
Outputs:
- coefficients: float32 [4096, 4096], P('curve', 'tm')
- scores: float32 [4096, 64], P('curve')
- sketch: float32 [4096, 64], P('tm', 'curve')
The draws below stay inside these ranges and needn't reach their ends.
All inputs are finite; a program needn't handle non-finite values.
Results may differ from the reference program's by a relative error of at most 0.0002.
Values sent between devices are 32-bit elements; how exact they have to be, the bound alone decides.
No kernel may reach another device: no remote copies, remote signals or barrier semaphores. Data moves between devices by JAX's collectives and lax.ppermute only.
A program may use at most 192 MiB of HBM per device.

```python
import math
import jax
import jax.numpy as jnp
from jax import lax

K = 4096
SPB = 16
RANK = 64
ITERS = 4
CURVES = 4096
SAMPLES = 65536


def draw_samples(key, part):
    first_key, second_key = jax.random.split(jax.random.fold_in(key, 71))
    ramp = 1.0 + 2.0 * jnp.arange(CURVES, dtype=jnp.float32) / max(CURVES - 1, 1)
    noise = jax.random.truncated_normal(first_key, -6.0, 6.0, (CURVES, SAMPLES), jnp.float32)
    common = jax.random.truncated_normal(second_key, -6.0, 6.0, (SAMPLES,), jnp.float32)
    return jnp.clip(noise + ramp[:, None] * common[None, :], -30.0, 30.0)


def block_scale(own_key, dims, cuts, least, largest):
    level, own = 1.0, jax.random.fold_in(own_key, 6)
    for dim, shards_of in cuts:
        steps = jnp.exp(jax.random.uniform(jax.random.fold_in(own, dim), (shards_of,), jnp.float32, least / len(cuts), largest / len(cuts)))
        level = level * jnp.repeat(steps, dims[dim] // shards_of).reshape([-1 if axis == dim else 1 for axis in range(len(dims))])
    return level


def gaussian(rng, shape, deviation, reach, cuts=(), kind=jnp.bfloat16):
    values = jax.random.normal(rng, shape, jnp.float32) * deviation
    if len(cuts) > 0:
        values = block_scale(rng, shape, cuts, -0.22, 0.18) * values
    return jnp.clip(values, min=-reach, max=reach).astype(kind)


def setup_inputs(seed: int = 0) -> dict:
    splits = jax.random.split(jax.random.key(seed), 5)
    return {
        "samples": draw_samples(jax.random.fold_in(splits[4], 71), 0),
        "smoothing": jnp.clip(jnp.exp(math.log(20.0) - 3.6888795 * jax.random.uniform(splits[1], (CURVES,), jnp.float32) ** block_scale(splits[1], (CURVES,), ((0, 16),), -0.2, 0.2)), 0.5, 20.0),
        "test_matrix": gaussian(splits[2], (K, RANK), RANK ** -0.5, 0.75, ((0, 2),), jnp.float32),
        "sketch_prev": gaussian(splits[3], (K, RANK), 0.2, 1.2, ((0, 2), (1, 16)), jnp.float32),
    }


damping = 0.45


def weight_table():
    frac = (jnp.arange(SPB, dtype=jnp.float32) + 0.5) / SPB
    pieces = [frac ** 3 / 6.0, (-3.0 * frac ** 3 + 3.0 * frac ** 2 + 3.0 * frac + 1.0) / 6.0, (3.0 * frac ** 3 - 6.0 * frac ** 2 + 4.0) / 6.0, (1.0 - frac) ** 3 / 6.0]
    return jnp.stack(pieces) / SPB


def relax_sweep(widened, target, smooth_col, index_wide, total_basis):
    second = widened[:, 2:] - 2.0 * widened[:, 1:-1] + widened[:, :-2]
    in_range = (index_wide[:-2] >= 0) & (index_wide[:-2] <= total_basis - 3)
    second = jnp.where(in_range[None, :], second, 0.0)
    bending = second[:, 2:] - 2.0 * second[:, 1:-1] + second[:, :-2]
    interior = widened[:, 2:-2]
    column_index = index_wide[2:-2]
    penalty_diag = (column_index <= total_basis - 3).astype(jnp.float32) + 4.0 * ((column_index >= 1) & (column_index <= total_basis - 2)).astype(jnp.float32) + (column_index >= 2).astype(jnp.float32)
    return interior + damping * (target - interior - smooth_col * bending) / (1.0 + smooth_col * penalty_diag)


def reference(samples, smoothing, test_matrix, sketch_prev):
    row_count = samples.shape[0]
    blocks = samples.reshape(row_count, K, SPB)
    segment_sums = jnp.einsum("cgq,mq->mcg", blocks, weight_table(), precision=lax.Precision.HIGHEST)
    padded = jnp.pad(segment_sums, ((0, 0), (0, 0), (3, 3)))
    proj = padded[0, :, 0:K] + padded[1, :, 1:K + 1] + padded[2, :, 2:K + 2] + padded[3, :, 3:K + 3]
    smooth_col = smoothing[:, None]
    index_wide = jnp.arange(K + 4, dtype=jnp.int32) - 2
    coefficients = proj
    for sweep_number in range(ITERS):
        widened = jnp.pad(coefficients, ((0, 0), (2, 2)))
        coefficients = relax_sweep(widened, proj, smooth_col, index_wide, K)
    column_mean = jnp.sum(coefficients, axis=0) / CURVES
    centered = coefficients - column_mean[None, :]
    scores = jnp.dot(centered, test_matrix, precision=lax.Precision.HIGHEST, preferred_element_type=jnp.float32)
    sketch_part = jnp.einsum("ck,cr->kr", centered, scores, precision=lax.Precision.HIGHEST) / CURVES
    return coefficients, scores, sketch_prev + sketch_part
```

```python
import functools

import jax
import jax.numpy as jnp
import numpy as np
from jax import lax
from jax.experimental import pallas as pl
from jax.experimental.pallas import tpu as pltpu
from jax.sharding import PartitionSpec as P

SPB = 16
ITERS = 4
LANES = 128
TILE = LANES * SPB
SPILL = TILE - 2 * LANES
ZONE_LOW = 8
ZONE_HIGH = 16
EDGE = 24

damping = 0.45


def banded_weights():
    frac = (np.arange(SPB, dtype=np.float64) + 0.5) / SPB
    table = np.stack([
        frac**3 / 6.0,
        (-3.0 * frac**3 + 3.0 * frac**2 + 3.0 * frac + 1.0) / 6.0,
        (3.0 * frac**3 - 6.0 * frac**2 + 4.0) / 6.0,
        (1.0 - frac) ** 3 / 6.0,
    ]) / SPB
    weights = np.zeros((TILE, LANES), np.float32)
    for segment in range(LANES):
        for piece in range(4):
            column = (segment + 3 - piece) % LANES
            weights[segment * SPB : (segment + 1) * SPB, column] = table[piece]
    high = weights.astype(jnp.bfloat16)
    low = (weights - high.astype(np.float32)).astype(jnp.bfloat16)
    return jnp.asarray(np.concatenate([high, low], axis=1))


def split_bf16(value):
    high = value.astype(jnp.bfloat16)
    return high, (value - high.astype(jnp.float32)).astype(jnp.bfloat16)


def dot32(a, b):
    return jnp.dot(a, b, preferred_element_type=jnp.float32)


def from_left(tiles, lane):
    turned = [pltpu.roll(t, 1, 1) for t in tiles]
    before = [jnp.zeros_like(turned[0])] + turned[:-1]
    return [jnp.where(lane == 0, p, t) for p, t in zip(before, turned)]


def from_right(tiles, lane):
    turned = [pltpu.roll(t, LANES - 1, 1) for t in tiles]
    after = turned[1:] + [jnp.zeros_like(turned[0])]
    return [jnp.where(lane == LANES - 1, n, t) for n, t in zip(after, turned)]


def second_difference(tiles, lane):
    left, right = from_left(tiles, lane), from_right(tiles, lane)
    return [(l + r) - (t + t) for l, t, r in zip(left, tiles, right)]


def relax_rows(tiles, smooth, lane):
    count = len(tiles)
    diag_first = jnp.where(lane == 0, 1.0, jnp.where(lane == 1, 5.0, 6.0))
    diag_last = jnp.where(lane == LANES - 1, 1.0, jnp.where(lane == LANES - 2, 5.0, 6.0))
    factor = [damping / (1.0 + 6.0 * smooth)] * count
    factor[0] = damping / (1.0 + smooth * diag_first)
    factor[-1] = damping / (1.0 + smooth * diag_last)
    if count == 1:
        factor[0] = damping / (1.0 + smooth * jnp.minimum(diag_first, diag_last))
    keep = {id(f): 1.0 - f for f in factor}
    pull = {id(f): f * smooth for f in factor}
    pulled = [f * t for f, t in zip(factor, tiles)]
    state = tiles
    for _ in range(ITERS):
        second = second_difference(state, lane)
        second[0] = jnp.where(lane == 0, 0.0, second[0])
        second[-1] = jnp.where(lane == LANES - 1, 0.0, second[-1])
        bending = second_difference(second, lane)
        state = [
            keep[id(f)] * t + p - pull[id(f)] * b
            for f, t, p, b in zip(factor, state, pulled, bending)
        ]
    return state


def curve_kernel(steps, step_rows, x_ref, smooth_ref, test_ref, w_ref, c_ref, msg_ref,
                 lhs_ref, main_ref, last_ref, smooth_cols, test_cols, c_high, c_low, scored, edge_ref):
    step = pl.program_id(0)
    blocks = x_ref.shape[1] // TILE
    rows = smooth_ref.shape[1]
    rank = test_ref.shape[0]
    has_left = lax.axis_index("tm") > 0
    has_right = lax.axis_index("tm") < lax.axis_size("tm") - 1
    lane = lax.broadcasted_iota(jnp.int32, (8, LANES), 1)

    @pl.when(step == 0)
    def _():
        for at in range(0, rows, LANES):
            part = jnp.broadcast_to(smooth_ref[:, at : at + LANES], (LANES, LANES))
            smooth_cols[at : at + LANES, :] = part.T
        for b in range(blocks):
            part = test_ref[:, b * LANES : (b + 1) * LANES]
            high, low = split_bf16(part)
            both = jnp.concatenate([high.astype(jnp.float32), low.astype(jnp.float32)], axis=0)
            test_cols[b * LANES : (b + 1) * LANES, :] = both.T.astype(jnp.bfloat16)

    def relax_step():
        slot = lax.rem(step + 1, 2)
        first_row = pl.multiple_of(jnp.maximum(step - 1, 0) * step_rows, step_rows)
        for group in range(0, step_rows, 16):
            halves = []
            for sub in (group, group + 8):
                at = pl.ds(pl.multiple_of(first_row + sub, 8), 8)
                smooth = smooth_cols[at, :]
                last = [last_ref[slot, b * step_rows + sub : b * step_rows + sub + 8, :] for b in range(blocks)]
                before = [jnp.zeros_like(last[0])] + last[:-1]
                tiles = [
                    main_ref[slot, b * step_rows + sub : b * step_rows + sub + 8, :]
                    + jnp.where(lane < LANES // 2, before[b], last[b])
                    for b in range(blocks)
                ]
                edge_right = jnp.where(
                    lane < ZONE_HIGH,
                    pltpu.roll(tiles[-1], ZONE_HIGH, 1),
                    pltpu.roll(last[-1], ZONE_HIGH, 1),
                )
                edge_ref[at, :] = jnp.where(has_right, edge_right, tiles[0])
                out = relax_rows(tiles, smooth, lane)
                for b in range(blocks):
                    c_ref[sub : sub + 8, b * LANES : (b + 1) * LANES] = out[b]
                out[0] = jnp.where(jnp.logical_and(has_left, lane < ZONE_HIGH), 0.0, out[0])
                out[-1] = jnp.where(
                    jnp.logical_and(has_right, lane >= LANES - ZONE_LOW), 0.0, out[-1]
                )
                halves.append(out)
            at = pl.ds(pl.multiple_of(first_row + group, 16), 16)
            for b in range(blocks):
                high, low = split_bf16(jnp.concatenate([halves[0][b], halves[1][b]], axis=0))
                c_high[at, b * LANES : (b + 1) * LANES] = high
                c_low[at, b * LANES : (b + 1) * LANES] = low

    def project_step():
        slot = lax.rem(step, 2)
        for b in range(blocks):
            high, low = split_bf16(x_ref[:, b * TILE : (b + 1) * TILE])
            lhs_ref[b * step_rows : (b + 1) * step_rows, :TILE] = high
            lhs_ref[b * step_rows : (b + 1) * step_rows, TILE:] = low
        most = dot32(lhs_ref[:, :SPILL], w_ref[:SPILL, :]) + dot32(
            lhs_ref[:, TILE : TILE + SPILL], w_ref[:SPILL, :]
        )
        main_ref[slot] = most[:, :LANES] + most[:, LANES:]
        rest = dot32(lhs_ref[:, SPILL:TILE], w_ref[SPILL:, :]) + dot32(
            lhs_ref[:, TILE + SPILL :], w_ref[SPILL:, :]
        )
        last_ref[slot] = rest[:, :LANES] + rest[:, LANES:]

    @pl.when(step < steps)
    def _():
        relax_step()
        project_step()

    @pl.when(step == steps)
    def _():
        relax_step()
        scored[...] = dot32(c_high[...], test_cols[...]) + dot32(c_low[...], test_cols[...])
        for at in range(0, rows, LANES):
            turned = scored[at : at + LANES, :].T
            msg_ref[:rank, at : at + LANES] = turned[:rank] + turned[rank:]
            msg_ref[rank : rank + EDGE, at : at + LANES] = edge_ref[at : at + LANES, :].T[:EDGE]
        low_zone = padded_turn(test_ref[:, test_ref.shape[1] - LANES :])[LANES - ZONE_LOW :]
        high_zone = padded_turn(test_ref[:, :LANES])
        base = rank + EDGE
        msg_ref[base:, :] = jnp.zeros_like(msg_ref[base:, :])
        msg_ref[base:, :LANES] = jnp.where(has_right, low_zone, high_zone[:8])
        msg_ref[base:, LANES : 2 * LANES] = high_zone[8:16]


def padded_turn(part):
    fill = jnp.zeros((LANES - part.shape[0], LANES), part.dtype)
    return jnp.concatenate([part, fill], axis=0).T


def curve_stage(samples, smooth_row, test_t, step_rows):
    rows, width = samples.shape
    rank, basis = test_t.shape
    steps = rows // step_rows
    stacked = step_rows * (width // TILE)
    f32, bf16 = jnp.float32, jnp.bfloat16
    return pl.pallas_call(
        functools.partial(curve_kernel, steps, step_rows),
        grid=(steps + 1,),
        out_shape=(
            jax.ShapeDtypeStruct((rows, basis), f32),
            jax.ShapeDtypeStruct((rank + EDGE + 8, rows), f32),
        ),
        in_specs=[
            pl.BlockSpec((step_rows, width), lambda i: (jnp.minimum(i, steps - 1), 0)),
            pl.BlockSpec((1, rows), lambda i: (0, 0)),
            pl.BlockSpec((rank, basis), lambda i: (0, 0)),
            pl.BlockSpec((TILE, 2 * LANES), lambda i: (0, 0)),
        ],
        out_specs=(
            pl.BlockSpec((step_rows, basis), lambda i: (jnp.maximum(i - 1, 0), 0)),
            pl.BlockSpec((rank + EDGE + 8, rows), lambda i: (0, 0)),
        ),
        scratch_shapes=[
            pltpu.VMEM((stacked, 2 * TILE), bf16),
            pltpu.VMEM((2, stacked, LANES), f32),
            pltpu.VMEM((2, stacked, LANES), f32),
            pltpu.VMEM((rows, LANES), f32),
            pltpu.VMEM((basis, 2 * rank), bf16),
            pltpu.VMEM((rows, basis), bf16),
            pltpu.VMEM((rows, basis), bf16),
            pltpu.VMEM((rows, 2 * rank), f32),
            pltpu.VMEM((rows, LANES), f32),
        ],
        compiler_params=pltpu.CompilerParams(
            dimension_semantics=("arbitrary",), vmem_limit_bytes=40 * 1024 * 1024
        ),
        cost_estimate=pl.CostEstimate(
            flops=4 * rows * width * 2 * LANES, bytes_accessed=4 * rows * width, transcendentals=0
        ),
        name="curves",
    )(samples, smooth_row, test_t, banded_weights())


def relax_strip(strip, smooth_row):
    factor = damping / (1.0 + 6.0 * smooth_row)
    pull = factor * smooth_row
    height = strip.shape[0]
    pulled = factor * strip
    state = strip

    def difference(v):
        return pltpu.roll(v, 1, 0) + pltpu.roll(v, height - 1, 0) - (v + v)

    for _ in range(ITERS):
        state = (1.0 - factor) * state + pulled - pull * difference(difference(state))
    return state


def swapped(value, block, flip):
    parts = [value[at : at + block] for at in range(0, value.shape[0], block)]
    other = [parts[k ^ 1] for k in range(len(parts))]
    return jnp.where(flip, jnp.concatenate(other, axis=0), value)


def exchange_order(value, order, index):
    count = 1 << len(order)
    block = value.shape[0] // count
    owner = [sum(b for k, b in enumerate(order) if p >> (len(order) - 1 - k) & 1) for p in range(count)]
    value = jnp.concatenate([value[q * block : (q + 1) * block] for q in owner], axis=0)
    for k, bit in enumerate(order):
        value = swapped(value, value.shape[0] >> (k + 1), (index & bit) != 0)
    return value


def sketch_kernel(order, own_ref, came_ref, smooth_ref, c_in, c_ref, keep_ref, send_ref, total_ref,
                  c_all, tile_ref, load_sem, store_sem):
    rows, basis = c_in.shape
    rank = total_ref.shape[0]
    tiles = basis // LANES
    half = rank // 2
    has_left = lax.axis_index("tm") > 0
    load = pltpu.make_async_copy(c_in, c_all, load_sem)
    load.start()

    own, came = own_ref[...], came_ref[...]
    is_low = jnp.logical_not(has_left)
    low = jnp.where(is_low, own, came)
    high = jnp.where(is_low, came, own)
    fill = jnp.zeros((EDGE - ZONE_LOW, rows), jnp.float32)
    strip = jnp.concatenate([low[rank : rank + EDGE], fill], axis=0) + jnp.concatenate(
        [fill, high[rank : rank + EDGE]], axis=0
    )
    fixed = relax_strip(strip, smooth_ref[...])[ZONE_LOW : ZONE_LOW + EDGE]
    base = rank + EDGE
    zone_test = jnp.concatenate(
        [low[base:, :LANES], high[base:, :LANES], high[base:, LANES : 2 * LANES]], axis=0
    )[:, :rank]
    zone_scores = lax.dot_general(
        zone_test, fixed, (((0,), (0,)), ((), ())),
        precision=lax.Precision.HIGHEST, preferred_element_type=jnp.float32,
    )
    total = own[:rank] + came[:rank] + zone_scores
    total_ref[...] = total

    placed = jnp.where(
        has_left,
        jnp.concatenate([fixed[ZONE_LOW:], jnp.zeros((LANES - ZONE_HIGH, rows), jnp.float32)], axis=0),
        jnp.concatenate([jnp.zeros((LANES - ZONE_LOW, rows), jnp.float32), fixed[:ZONE_LOW]], axis=0),
    )
    lane = lax.broadcasted_iota(jnp.int32, (LANES, LANES), 1)
    first, past = jnp.where(has_left, 0, LANES - ZONE_LOW), jnp.where(has_left, ZONE_HIGH, LANES)
    fix_lane = jnp.logical_and(lane >= first, lane < past)
    edge = pl.multiple_of(jnp.where(has_left, 0, basis - LANES), LANES)

    mean_score = jnp.mean(total, axis=1, keepdims=True)
    spread = jnp.broadcast_to(mean_score, (rank, LANES))
    score_row = padded_turn(spread)[:8]
    index = lax.axis_index("curve")
    spread = exchange_order(spread, order, index)
    lhs_high, lhs_low = split_bf16(exchange_order(total - mean_score, order, index))
    lhs = jnp.concatenate([lhs_high, lhs_low], axis=0)

    load.wait()
    for at in range(0, rows, LANES):
        here = c_all[at : at + LANES, pl.ds(edge, LANES)]
        here = jnp.where(fix_lane, placed[:, at : at + LANES].T, here)
        tile_ref[at : at + LANES, :] = here
        c_all[at : at + LANES, pl.ds(edge, LANES)] = here
    store = pltpu.make_async_copy(tile_ref, c_ref.at[:, pl.ds(edge, LANES)], store_sem)
    store.start()

    for b in range(tiles):
        block = c_all[:, b * LANES : (b + 1) * LANES]
        mean = jnp.mean(block, axis=0, keepdims=True)
        rhs_high, rhs_low = split_bf16(block - mean)
        out = dot32(lhs, rhs_high)
        out = out[:rank] + out[rank:] + dot32(lhs_high, rhs_low)
        keep_ref[b * half : (b + 1) * half, :] = out[:half]
        send_ref[b * half : (b + 1) * half, :] = out[half:]
        at = (tiles + 1) * half + b
        keep_ref[at : at + 1, :] = mean
        send_ref[at : at + 1, :] = mean
    at = tiles * half
    keep_ref[at : at + half, :] = spread[:half]
    send_ref[at : at + half, :] = spread[half:]
    at = (tiles + 1) * half + tiles
    keep_ref[at:, :] = score_row
    send_ref[at:, :] = score_row
    store.wait()


def sketch_stage(own, came, smooth_row, coefficients, rank, order):
    rows, basis = coefficients.shape
    tiles = basis // LANES
    half = rank // 2
    f32 = jnp.float32
    packed = jax.ShapeDtypeStruct(((tiles + 1) * half + tiles + 8, LANES), f32)
    vmem, anywhere = pl.BlockSpec(memory_space=pltpu.VMEM), pl.BlockSpec(memory_space=pl.ANY)
    return pl.pallas_call(
        functools.partial(sketch_kernel, order),
        out_shape=(
            jax.ShapeDtypeStruct((rows, basis), f32), packed, packed,
            jax.ShapeDtypeStruct((rank, rows), f32),
        ),
        in_specs=[vmem, vmem, vmem, anywhere],
        out_specs=(anywhere, vmem, vmem, vmem),
        scratch_shapes=[
            pltpu.VMEM((rows, basis), f32),
            pltpu.VMEM((rows, LANES), f32),
            pltpu.SemaphoreType.DMA,
            pltpu.SemaphoreType.DMA,
        ],
        input_output_aliases={3: 0},
        compiler_params=pltpu.CompilerParams(vmem_limit_bytes=16 * 1024 * 1024),
        cost_estimate=pl.CostEstimate(
            flops=6 * rows * basis * rank, bytes_accessed=4 * rows * basis, transcendentals=0
        ),
        name="sketch_part",
    )(own, came, smooth_row, coefficients)


def unpack(packed, tiles, height):
    moment = packed[: tiles * height].reshape(tiles, height, LANES)
    score = packed[tiles * height : (tiles + 1) * height]
    rest = packed[(tiles + 1) * height :]
    return moment, score, rest


def merged(keep, came, tiles, height, count):
    moment, score, rest = unpack(keep, tiles, height)
    moment_2, score_2, rest_2 = unpack(came, tiles, height)
    apart = rest[:tiles] - rest_2[:tiles]
    moment = moment + moment_2 + (0.5 * count) * apart[:, None, :] * (score - score_2)[None]
    return moment, 0.5 * (score + score_2), 0.5 * (rest + rest_2)


def packed_half(moment, score, rest, which):
    height = moment.shape[1] // 2
    part = slice(which * height, (which + 1) * height)
    moment = moment[:, part].reshape(-1, LANES)
    return jnp.concatenate([moment, score[part], rest], axis=0)


def fast_body(samples, smoothing, test_matrix, sketch_prev):
    rows, basis = samples.shape[0], test_matrix.shape[0]
    rank = test_matrix.shape[1]
    tiles = basis // LANES
    groups = lax.axis_size("curve")
    order = [1 << k for k in range(groups.bit_length() - 1)]
    smooth_row = smoothing[None, :]
    coefficients, message = curve_stage(samples, smooth_row, test_matrix.T, 32)
    came = lax.ppermute(message, "tm", [(0, 1), (1, 0)])
    coefficients, keep, send, total = sketch_stage(message, came, smooth_row, coefficients, rank, order)
    height, count = rank // 2, rows
    for bit in order:
        came = lax.ppermute(send, "curve", [(i, i ^ bit) for i in range(groups)])
        moment, score, rest = merged(keep, came, tiles, height, count)
        count *= 2
        if bit != order[-1]:
            keep = packed_half(moment, score, rest, 0)
            send = packed_half(moment, score, rest, 1)
            height //= 2
    score_mean = rest[tiles, :rank]
    scores = (total - score_mean[:, None]).T
    sketch = sketch_prev + moment.transpose(0, 2, 1).reshape(basis, height) / count
    return coefficients, scores, sketch


def passed_along(block, axis, distance):
    devices = range(lax.axis_size(axis))
    route = [(i - distance, i) for i in devices if i - distance in devices]
    return lax.ppermute(block, axis, route)


def padded_2(block, sides, width):
    for axis, dim in sides:
        count = lax.axis_size(axis)
        forward = [(i, i + 1) for i in range(count - 1)]
        backward = [(target, source) for source, target in forward]
        low = lax.ppermute(
            lax.slice_in_dim(block, block.shape[dim] - width, None, axis=dim), axis, forward
        )
        high = lax.ppermute(lax.slice_in_dim(block, 0, width, axis=dim), axis, backward)
        block = jnp.concatenate([low, block, high], axis=dim)
    return block


def weight_table():
    frac = (jnp.arange(SPB, dtype=jnp.float32) + 0.5) / SPB
    pieces = [
        frac**3 / 6.0,
        (-3.0 * frac**3 + 3.0 * frac**2 + 3.0 * frac + 1.0) / 6.0,
        (3.0 * frac**3 - 6.0 * frac**2 + 4.0) / 6.0,
        (1.0 - frac) ** 3 / 6.0,
    ]
    return jnp.stack(pieces) / SPB


def relax_sweep(widened, target, smooth_col, index_wide, total_basis):
    second = widened[:, 2:] - 2.0 * widened[:, 1:-1] + widened[:, :-2]
    in_range = (index_wide[:-2] >= 0) & (index_wide[:-2] <= total_basis - 3)
    second = jnp.where(in_range[None, :], second, 0.0)
    bending = second[:, 2:] - 2.0 * second[:, 1:-1] + second[:, :-2]
    interior = widened[:, 2:-2]
    column_index = index_wide[2:-2]
    penalty_diag = (
        (column_index <= total_basis - 3).astype(jnp.float32)
        + 4.0 * ((column_index >= 1) & (column_index <= total_basis - 2)).astype(jnp.float32)
        + (column_index >= 2).astype(jnp.float32)
    )
    return interior + damping * (target - interior - smooth_col * bending) / (
        1.0 + smooth_col * penalty_diag
    )


def plain_body(samples, smoothing, test_matrix, sketch_prev):
    row_count = samples.shape[0]
    basis_width = samples.shape[1] // SPB
    blocks = samples.reshape(row_count, basis_width, SPB)
    segment_sums = jnp.einsum(
        "cgq,mq->mcg", blocks, weight_table(), precision=lax.Precision.HIGHEST
    )
    padded = jnp.pad(segment_sums, ((0, 0), (0, 0), (3, 3)))
    extended = (
        padded[0, :, 0 : basis_width + 3]
        + padded[1, :, 1 : basis_width + 4]
        + padded[2, :, 2 : basis_width + 5]
        + padded[3, :, 3 : basis_width + 6]
    )
    spilled = extended[:, basis_width:]
    arrived = passed_along(spilled, "tm", 1)
    proj = jnp.concatenate([extended[:, :3] + arrived, extended[:, 3:basis_width]], axis=1)
    total_basis = basis_width * lax.axis_size("tm")
    first_column = lax.axis_index("tm") * basis_width
    smooth_col = smoothing[:, None]
    margin = 2 * ITERS
    proj_wide = padded_2(proj, (("tm", 1),), margin)
    coefficients = proj_wide
    for sweep_number in range(ITERS):
        margin_now = margin - 2 * sweep_number
        index_wide = (
            first_column - margin_now + jnp.arange(basis_width + 2 * margin_now, dtype=jnp.int32)
        )
        offset = 2 * sweep_number + 2
        target = proj_wide[:, offset : offset + basis_width + 2 * margin_now - 4]
        coefficients = relax_sweep(coefficients, target, smooth_col, index_wide, total_basis)
    curve_total = row_count * lax.axis_size("curve")
    totals = lax.psum(jnp.sum(coefficients, axis=0), "curve")
    column_mean = totals / curve_total
    centered = coefficients - column_mean[None, :]
    partial_value = jnp.dot(
        centered, test_matrix, precision=lax.Precision.HIGHEST, preferred_element_type=jnp.float32
    )
    scores = lax.psum(partial_value, "tm")
    sketch_part = (
        jnp.einsum("ck,cr->kr", centered, scores, precision=lax.Precision.HIGHEST) / curve_total
    )
    owned_part = lax.psum_scatter(sketch_part, "curve", scatter_dimension=1, tiled=True)
    return (coefficients, scores, sketch_prev + owned_part)


def fits(mesh):
    groups = mesh.shape["curve"]
    return mesh.shape["tm"] == 2 and groups > 1 and groups & (groups - 1) == 0


def solution(mesh):
    placed = (P("curve", "tm"), P("curve"), P("tm", None), P("tm", "curve"))
    return jax.shard_map(
        fast_body if fits(mesh) else plain_body,
        mesh=mesh,
        in_specs=placed,
        out_specs=(P("curve", "tm"), P("curve", None), P("tm", "curve")),
        check_vma=False,
    )
```

```python
import functools

import jax
import jax.numpy as jnp
import numpy as np
from jax import lax
from jax.experimental import pallas as pl
from jax.experimental.pallas import tpu as pltpu
from jax.sharding import PartitionSpec as P

SPB = 16
ITERS = 4
LANES = 128
TILE = LANES * SPB
CHUNK = 256
HEAD = 24
DEPTH = 5
WINDOW = HEAD + LANES
ZONE_LOW = 8
ZONE_HIGH = 16
EDGE = 24

RADIX_BITS = 2

damping = 0.45


def banded_weights():
    frac = (np.arange(SPB, dtype=np.float64) + 0.5) / SPB
    table = np.stack([
        frac**3 / 6.0,
        (-3.0 * frac**3 + 3.0 * frac**2 + 3.0 * frac + 1.0) / 6.0,
        (3.0 * frac**3 - 6.0 * frac**2 + 4.0) / 6.0,
        (1.0 - frac) ** 3 / 6.0,
    ]) / SPB
    weights = np.zeros((CHUNK, LANES), np.float32)
    for segment in range(CHUNK // SPB):
        for piece in range(4):
            weights[segment * SPB : (segment + 1) * SPB, segment + 3 - piece] = table[piece]
    return jnp.asarray(weights)


def split_bf16(value):
    high = value.astype(jnp.bfloat16)
    return high, (value - high.astype(jnp.float32)).astype(jnp.bfloat16)


def dot32(a, b):
    return jnp.dot(a, b, preferred_element_type=jnp.float32)


def sweep_factors(smooth, diag):
    factor = damping / (1.0 + smooth * diag)
    pull = factor * smooth
    return 1.0 - factor - 6.0 * pull, 4.0 * pull, pull, factor


def relaxed(at_hand, near, far, target, factors):
    own, four, one, factor = factors
    return own * at_hand + factor * target + four * near - one * far


def curve_kernel(x_all, smooth_ref, test_all, band_all, c_all, msg_ref, w_ref, main_ref, last_ref, proj_ref,
                 state_ref, done_ref, scored, strip_ref, x_ref, x_sems, test_ref, test_sem, c_ref, c_sems, band_ref, band_sem):
    rows, basis = c_all.shape
    blocks = basis // LANES
    rank = test_ref.shape[0]
    halves = rows // LANES
    height = WINDOW
    base = rank + EDGE
    has_left = lax.axis_index("tm") > 0
    has_right = lax.axis_index("tm") < lax.axis_size("tm") - 1
    sub = lax.broadcasted_iota(jnp.int32, (8, LANES), 0)

    def tile_at(which):
        return pl.ds(pl.multiple_of(which * LANES, LANES), LANES)

    def incoming(which):
        at = pl.ds(pl.multiple_of(which * TILE, TILE), TILE)
        slot = lax.rem(which, DEPTH)
        return pltpu.make_async_copy(x_all.at[:, at], x_ref.at[slot], x_sems.at[slot])

    def outgoing(which):
        at = tile_at(which)
        return pltpu.make_async_copy(c_ref.at[:, at], c_all.at[:, at], c_sems.at[which])

    def project(step, between):
        slot = lax.rem(step, 2)

        def chunk_dot(r):
            high, low = split_bf16(x_ref[lax.rem(step, DEPTH), :, r * CHUNK : (r + 1) * CHUNK])
            w = w_ref[r * CHUNK : (r + 1) * CHUNK, :]
            return dot32(high, w) + dot32(low, w)

        count = TILE // CHUNK
        for _ in between:
            pass
        rest = chunk_dot(count - 1)
        last_ref[slot] = rest[:, :LANES] + rest[:, LANES:]
        most = None
        for r in range(count - 1):
            part = chunk_dot(r)
            most = part if most is None else most + part
        for _ in between:
            pass
        main_ref[slot] = most[:, :LANES] + most[:, LANES:]

    def relax(block, is_end=False):
        slot, before = lax.rem(block + 2, 2), lax.rem(block + 1, 2)
        is_first = block == 0
        write_at = jnp.maximum(block, 0) * LANES
        for h in range(halves):
            cols = slice(h * LANES, (h + 1) * LANES)
            proj_ref[h, 8:HEAD, :] = proj_ref[h, LANES + 8 : LANES + HEAD, :]
            wide = lax.broadcasted_iota(jnp.int32, (LANES, LANES), 1)
            earlier = jnp.where(is_first, 0.0, last_ref[before, cols, :])
            here = main_ref[slot, cols, :] + jnp.where(wide < LANES // 2, earlier, last_ref[slot, cols, :])
            turned = here.T
            proj_ref[h, HEAD : HEAD + LANES, :] = turned
            if not is_end:
                strip_ref[h] = jnp.where(is_first, turned[:EDGE], strip_ref[h])
            else:
                spilled = last_ref[slot, cols, :].T[:8]
                ending = jnp.concatenate([turned[LANES - ZONE_HIGH :], spilled], axis=0)
                strip_ref[h] = jnp.where(has_right, ending, strip_ref[h])

            smooth = jnp.broadcast_to(smooth_ref[:, cols], (8, LANES))
            starting = closing = inner = sweep_factors(smooth, 6.0)
            if not is_end:
                diag = jnp.where(sub == 0, 1.0, jnp.where(sub == 1, 5.0, 6.0))
                starting = sweep_factors(smooth, jnp.where(is_first, diag, 6.0))
            else:
                closing = sweep_factors(smooth, jnp.where(sub == 7, 1.0, jnp.where(sub == 6, 5.0, 6.0)))

            def ghosts(ref, lead):
                def row(at):
                    return jnp.broadcast_to(ref[(*lead, slice(at, at + 1), slice(None))], (8, LANES))

                if not is_end:
                    zero, one = row(HEAD), row(HEAD + 1)
                    ahead = (*lead, slice(HEAD - 8, HEAD), slice(None))
                    outside = jnp.where(sub == 7, 2.0 * zero - one, 3.0 * zero - 2.0 * one)
                    ref[ahead] = jnp.where(is_first, outside, ref[ahead])
                else:
                    zero, one = row(height - 1), row(height - 2)
                    ref[(*lead, slice(height, height + 8), slice(None))] = jnp.where(
                        sub == 0, 2.0 * zero - one, 3.0 * zero - 2.0 * one
                    )

            ghosts(proj_ref, (h,))
            source, lead = proj_ref, (h,)
            for sweep in range(ITERS):
                final = sweep == ITERS - 1

                def load(at):
                    return source[(*lead, slice(at, at + 8), slice(None))]

                values = []
                for at in range(16 if final else 8, height, 8):
                    value = relaxed(
                        load(at),
                        load(at - 1) + load(at + 1),
                        load(at - 2) + load(at + 2),
                        proj_ref[h, at : at + 8, :],
                        starting if at == HEAD else closing if at == height - 8 else inner,
                    )
                    if final:
                        done_ref[h, pl.ds(pl.multiple_of(write_at + at - 16, 8), 8), :] = value
                    else:
                        state_ref[sweep, h, at : at + 8, :] = value
                if not final:
                    ghosts(state_ref, (sweep, h))
                    source, lead = state_ref, (sweep, h)
                yield

    def finish(which, end=False):
        parts = []
        for h in range(halves):
            where = pl.multiple_of(which * LANES + 8, 8)
            part = done_ref[h, pl.ds(where, LANES), :]
            c_ref[h * LANES : (h + 1) * LANES, tile_at(which)] = part.T
            parts.append(part)
        test = test_ref[:, tile_at(which)]
        wide = lax.broadcasted_iota(jnp.int32, (rank, LANES), 1)
        if not end:
            left_zone = jnp.logical_and(has_left, which == 0)
            test = jnp.where(jnp.logical_and(left_zone, wide < ZONE_HIGH), 0.0, test)
        else:
            test = jnp.where(jnp.logical_and(has_right, wide >= LANES - ZONE_LOW), 0.0, test)
        test_high, test_low = split_bf16(test)
        high, low = split_bf16(jnp.concatenate(parts, axis=1))
        both = dot32(jnp.concatenate([test_high, test_low], axis=0), high)
        more = both[:rank] + both[rank:] + dot32(test_high, low)
        scored[...] = jnp.where(which == 0, 0.0, scored[...]) + more

    band_copy = pltpu.make_async_copy(band_all, band_ref, band_sem)
    band_copy.start()
    test_copy = pltpu.make_async_copy(test_all, test_ref, test_sem)
    for which in range(min(DEPTH - 1, blocks)):
        incoming(which).start()
        if which == 0:
            test_copy.start()
    band_copy.wait()
    for r in range(TILE // CHUNK):
        high, low = split_bf16(pltpu.roll(band_ref[...], r * (CHUNK // SPB), 1))
        w_ref[r * CHUNK : (r + 1) * CHUNK, :LANES] = high
        w_ref[r * CHUNK : (r + 1) * CHUNK, LANES:] = low
    test_copy.wait()

    @pl.loop(0, blocks)
    def _(step):
        @pl.when(step + DEPTH - 1 < blocks)
        def _():
            incoming(step + DEPTH - 1).start()

        incoming(step).wait()
        finish(jnp.maximum(step - 3, 0))
        project(step, relax(step - 1))

        @pl.when(step >= 3)
        def _():
            outgoing(step - 3).start()

    finish(blocks - 3)
    outgoing(blocks - 3).start()
    for _ in relax(blocks - 1, is_end=True):
        pass
    finish(blocks - 2)
    outgoing(blocks - 2).start()
    finish(blocks - 1, end=True)
    outgoing(blocks - 1).start()

    msg_ref[:rank, :] = scored[...]
    for h in range(halves):
        msg_ref[rank:base, h * LANES : (h + 1) * LANES] = strip_ref[h]
    low_zone = padded_turn(test_ref[:, basis - LANES :])[LANES - ZONE_LOW :]
    high_zone = padded_turn(test_ref[:, :LANES])
    msg_ref[base:, :] = jnp.zeros_like(msg_ref[base:, :])
    msg_ref[base:, :LANES] = jnp.where(has_right, low_zone, high_zone[:8])
    msg_ref[base:, LANES : 2 * LANES] = high_zone[8:16]
    for which in range(blocks):
        outgoing(which).wait()


def padded_turn(part):
    fill = jnp.zeros((LANES - part.shape[0], LANES), part.dtype)
    return jnp.concatenate([part, fill], axis=0).T


def curve_stage(samples, smooth_row, test_t):
    rows, width = samples.shape
    rank, basis = test_t.shape
    blocks, halves = basis // LANES, rows // LANES
    f32, bf16 = jnp.float32, jnp.bfloat16
    vmem, hbm = pl.BlockSpec(memory_space=pltpu.VMEM), pl.BlockSpec(memory_space=pltpu.HBM)
    return pl.pallas_call(
        curve_kernel,
        out_shape=(
            jax.ShapeDtypeStruct((rows, basis), f32),
            jax.ShapeDtypeStruct((rank + EDGE + 8, rows), f32),
        ),
        in_specs=[hbm, vmem, hbm, hbm],
        out_specs=(hbm, vmem),
        scratch_shapes=[
            pltpu.VMEM((TILE, 2 * LANES), bf16),
            pltpu.VMEM((2, rows, LANES), f32),
            pltpu.VMEM((2, rows, LANES), f32),
            pltpu.VMEM((halves, WINDOW + 8, LANES), f32),
            pltpu.VMEM((ITERS - 1, halves, WINDOW + 8, LANES), f32),
            pltpu.VMEM((halves, basis + LANES, LANES), f32),
            pltpu.VMEM((rank, rows), f32),
            pltpu.VMEM((halves, EDGE, LANES), f32),
            pltpu.VMEM((DEPTH, rows, TILE), f32),
            pltpu.SemaphoreType.DMA((DEPTH,)),
            pltpu.VMEM((rank, basis), f32),
            pltpu.SemaphoreType.DMA,
            pltpu.VMEM((rows, basis), f32),
            pltpu.SemaphoreType.DMA((blocks,)),
            pltpu.VMEM((CHUNK, LANES), f32),
            pltpu.SemaphoreType.DMA,
        ],
        compiler_params=pltpu.CompilerParams(
            vmem_limit_bytes=60 * 1024 * 1024,
        ),
        cost_estimate=pl.CostEstimate(
            flops=4 * rows * width * 2 * LANES, bytes_accessed=4 * rows * width, transcendentals=0
        ),
        name="curves",
    )(samples, smooth_row, test_t, banded_weights())


def relax_strip(strip, smooth_row):
    factor = damping / (1.0 + 6.0 * smooth_row)
    pull = factor * smooth_row
    height = strip.shape[0]
    pulled = factor * strip
    state = strip

    def difference(v):
        return pltpu.roll(v, 1, 0) + pltpu.roll(v, height - 1, 0) - (v + v)

    for _ in range(ITERS):
        state = (1.0 - factor) * state + pulled - pull * difference(difference(state))
    return state


def swapped(value, block, flip):
    parts = [value[at : at + block] for at in range(0, value.shape[0], block)]
    other = [parts[k ^ 1] for k in range(len(parts))]
    return jnp.where(flip, jnp.concatenate(other, axis=0), value)


def exchange_order(value, order, index):
    count = 1 << len(order)
    block = value.shape[0] // count
    owner = [sum(b for k, b in enumerate(order) if p >> (len(order) - 1 - k) & 1) for p in range(count)]
    value = jnp.concatenate([value[q * block : (q + 1) * block] for q in owner], axis=0)
    for k, bit in enumerate(order):
        value = swapped(value, value.shape[0] >> (k + 1), (index & bit) != 0)
    return value


def sketch_kernel(order, own_all, came_ref, smooth_ref, c_in, c_ref, keep_ref, send_ref, total_ref,
                  c_all, tile_ref, own_ref, own_sem, load_sem, store_sem):
    rows, basis = c_in.shape
    rank = total_ref.shape[0]
    tiles = basis // LANES
    half = rank // 2
    has_left = lax.axis_index("tm") > 0
    bring = pltpu.make_async_copy(own_all, own_ref, own_sem)
    bring.start()
    load = pltpu.make_async_copy(c_in, c_all, load_sem)
    load.start()
    bring.wait()

    own, came = own_ref[...], came_ref[...]
    is_low = jnp.logical_not(has_left)
    low = jnp.where(is_low, own, came)
    high = jnp.where(is_low, came, own)
    fill = jnp.zeros((EDGE - ZONE_LOW, rows), jnp.float32)
    strip = jnp.concatenate([low[rank : rank + EDGE], fill], axis=0) + jnp.concatenate(
        [fill, high[rank : rank + EDGE]], axis=0
    )
    fixed = relax_strip(strip, smooth_ref[...])[ZONE_LOW : ZONE_LOW + EDGE]
    base = rank + EDGE
    zone_test = jnp.concatenate(
        [low[base:, :LANES], high[base:, :LANES], high[base:, LANES : 2 * LANES]], axis=0
    )[:, :rank]
    zone_scores = lax.dot_general(
        zone_test, fixed, (((0,), (0,)), ((), ())),
        precision=lax.Precision.HIGHEST, preferred_element_type=jnp.float32,
    )
    total = own[:rank] + came[:rank] + zone_scores
    total_ref[...] = total

    placed = jnp.where(
        has_left,
        jnp.concatenate([fixed[ZONE_LOW:], jnp.zeros((LANES - ZONE_HIGH, rows), jnp.float32)], axis=0),
        jnp.concatenate([jnp.zeros((LANES - ZONE_LOW, rows), jnp.float32), fixed[:ZONE_LOW]], axis=0),
    )
    lane = lax.broadcasted_iota(jnp.int32, (LANES, LANES), 1)
    first, past = jnp.where(has_left, 0, LANES - ZONE_LOW), jnp.where(has_left, ZONE_HIGH, LANES)
    fix_lane = jnp.logical_and(lane >= first, lane < past)
    edge = pl.multiple_of(jnp.where(has_left, 0, basis - LANES), LANES)

    mean_score = jnp.mean(total, axis=1, keepdims=True)
    spread = jnp.broadcast_to(mean_score, (rank, LANES))
    score_row = padded_turn(spread)[:8]
    index = lax.axis_index("curve")
    spread = exchange_order(spread, order, index)
    lhs_high, lhs_low = split_bf16(exchange_order(total - mean_score, order, index))
    lhs = jnp.concatenate([lhs_high, lhs_low], axis=0)

    load.wait()
    for at in range(0, rows, LANES):
        here = c_all[at : at + LANES, pl.ds(edge, LANES)]
        here = jnp.where(fix_lane, placed[:, at : at + LANES].T, here)
        tile_ref[at : at + LANES, :] = here
        c_all[at : at + LANES, pl.ds(edge, LANES)] = here
    store = pltpu.make_async_copy(tile_ref, c_ref.at[:, pl.ds(edge, LANES)], store_sem)
    store.start()

    for b in range(tiles):
        block = c_all[:, b * LANES : (b + 1) * LANES]
        mean = jnp.mean(block, axis=0, keepdims=True)
        rhs_high, rhs_low = split_bf16(block - mean)
        out = dot32(lhs, rhs_high)
        out = out[:rank] + out[rank:] + dot32(lhs_high, rhs_low)
        keep_ref[b * half : (b + 1) * half, :] = out[:half]
        send_ref[b * half : (b + 1) * half, :] = out[half:]
        at = (tiles + 1) * half + b
        keep_ref[at : at + 1, :] = mean
        send_ref[at : at + 1, :] = mean
    at = tiles * half
    keep_ref[at : at + half, :] = spread[:half]
    send_ref[at : at + half, :] = spread[half:]
    at = (tiles + 1) * half + tiles
    keep_ref[at:, :] = score_row
    send_ref[at:, :] = score_row
    store.wait()


def sketch_stage(own, came, smooth_row, coefficients, rank, order):
    rows, basis = coefficients.shape
    tiles = basis // LANES
    half = rank // 2
    f32 = jnp.float32
    packed = jax.ShapeDtypeStruct(((tiles + 1) * half + tiles + 8, LANES), f32)
    vmem, hbm = pl.BlockSpec(memory_space=pltpu.VMEM), pl.BlockSpec(memory_space=pltpu.HBM)
    return pl.pallas_call(
        functools.partial(sketch_kernel, order),
        out_shape=(
            jax.ShapeDtypeStruct((rows, basis), f32), packed, packed,
            jax.ShapeDtypeStruct((rank, rows), f32),
        ),
        in_specs=[hbm, vmem, vmem, hbm],
        out_specs=(hbm, vmem, vmem, vmem),
        scratch_shapes=[
            pltpu.VMEM((rows, basis), f32),
            pltpu.VMEM((rows, LANES), f32),
            pltpu.VMEM(own.shape, f32),
            pltpu.SemaphoreType.DMA,
            pltpu.SemaphoreType.DMA,
            pltpu.SemaphoreType.DMA,
        ],
        input_output_aliases={3: 0},
        compiler_params=pltpu.CompilerParams(vmem_limit_bytes=16 * 1024 * 1024),
        cost_estimate=pl.CostEstimate(
            flops=6 * rows * basis * rank, bytes_accessed=4 * rows * basis, transcendentals=0
        ),
        name="sketch_part",
    )(own, came, smooth_row, coefficients)


def unpack(packed, tiles, height):
    moment = packed[: tiles * height].reshape(tiles, height, LANES)
    score = packed[tiles * height : (tiles + 1) * height]
    rest = packed[(tiles + 1) * height :]
    return moment, score, rest


def merged(one, other, count):
    moment, score, rest = one
    moment_2, score_2, rest_2 = other
    tiles = moment.shape[0]
    apart = rest[:tiles] - rest_2[:tiles]
    moment = moment + moment_2 + (0.5 * count) * apart[:, None, :] * (score - score_2)[None]
    return moment, 0.5 * (score + score_2), 0.5 * (rest + rest_2)


def packed_share(group, which, shares):
    moment, score, rest = group
    height = moment.shape[1] // shares
    part = slice(which * height, (which + 1) * height)
    return jnp.concatenate([moment[:, part].reshape(-1, LANES), score[part], rest], axis=0)


def exchanged(packed, groups, bits):
    return lax.ppermute(packed, "curve", [(i, i ^ bits) for i in range(groups)])


def fast_body(samples, smoothing, test_matrix, sketch_prev):
    rows, basis = samples.shape[0], test_matrix.shape[0]
    rank = test_matrix.shape[1]
    tiles = basis // LANES
    groups = lax.axis_size("curve")
    order = [1 << k for k in range(groups.bit_length() - 1)]
    smooth_row = smoothing[None, :]
    coefficients, message = curve_stage(samples, smooth_row, test_matrix.T)
    came = lax.ppermute(message, "tm", [(0, 1), (1, 0)])
    coefficients, keep, send, total = sketch_stage(message, came, smooth_row, coefficients, rank, order)
    height, count = rank // 2, rows
    came = exchanged(send, groups, order[0])
    group = merged(unpack(keep, tiles, height), unpack(came, tiles, height), count)
    count *= 2
    rest = order[1:]
    while rest:
        bits, rest = rest[:RADIX_BITS], rest[RADIX_BITS:]
        shares = 1 << len(bits)
        height //= shares
        parts = [unpack(packed_share(group, 0, shares), tiles, height)]
        for which in range(1, shares):
            partner = sum(b for k, b in enumerate(bits) if which >> (len(bits) - 1 - k) & 1)
            came = exchanged(packed_share(group, which, shares), groups, partner)
            parts.append(unpack(came, tiles, height))
        while len(parts) > 1:
            parts = [merged(parts[k], parts[k + 1], count) for k in range(0, len(parts), 2)]
            count *= 2
        group = parts[0]
    moment, _, rest = group
    score_mean = rest[tiles, :rank]
    scores = (total - score_mean[:, None]).T
    sketch = sketch_prev + moment.transpose(0, 2, 1).reshape(basis, height) / count
    return coefficients, scores, sketch


def passed_along(block, axis, distance):
    devices = range(lax.axis_size(axis))
    route = [(i - distance, i) for i in devices if i - distance in devices]
    return lax.ppermute(block, axis, route)


def padded_2(block, sides, width):
    for axis, dim in sides:
        count = lax.axis_size(axis)
        forward = [(i, i + 1) for i in range(count - 1)]
        backward = [(target, source) for source, target in forward]
        low = lax.ppermute(
            lax.slice_in_dim(block, block.shape[dim] - width, None, axis=dim), axis, forward
        )
        high = lax.ppermute(lax.slice_in_dim(block, 0, width, axis=dim), axis, backward)
        block = jnp.concatenate([low, block, high], axis=dim)
    return block


def weight_table():
    frac = (jnp.arange(SPB, dtype=jnp.float32) + 0.5) / SPB
    pieces = [
        frac**3 / 6.0,
        (-3.0 * frac**3 + 3.0 * frac**2 + 3.0 * frac + 1.0) / 6.0,
        (3.0 * frac**3 - 6.0 * frac**2 + 4.0) / 6.0,
        (1.0 - frac) ** 3 / 6.0,
    ]
    return jnp.stack(pieces) / SPB


def relax_sweep(widened, target, smooth_col, index_wide, total_basis):
    second = widened[:, 2:] - 2.0 * widened[:, 1:-1] + widened[:, :-2]
    in_range = (index_wide[:-2] >= 0) & (index_wide[:-2] <= total_basis - 3)
    second = jnp.where(in_range[None, :], second, 0.0)
    bending = second[:, 2:] - 2.0 * second[:, 1:-1] + second[:, :-2]
    interior = widened[:, 2:-2]
    column_index = index_wide[2:-2]
    penalty_diag = (
        (column_index <= total_basis - 3).astype(jnp.float32)
        + 4.0 * ((column_index >= 1) & (column_index <= total_basis - 2)).astype(jnp.float32)
        + (column_index >= 2).astype(jnp.float32)
    )
    return interior + damping * (target - interior - smooth_col * bending) / (
        1.0 + smooth_col * penalty_diag
    )


def plain_body(samples, smoothing, test_matrix, sketch_prev):
    row_count = samples.shape[0]
    basis_width = samples.shape[1] // SPB
    blocks = samples.reshape(row_count, basis_width, SPB)
    segment_sums = jnp.einsum(
        "cgq,mq->mcg", blocks, weight_table(), precision=lax.Precision.HIGHEST
    )
    padded = jnp.pad(segment_sums, ((0, 0), (0, 0), (3, 3)))
    extended = (
        padded[0, :, 0 : basis_width + 3]
        + padded[1, :, 1 : basis_width + 4]
        + padded[2, :, 2 : basis_width + 5]
        + padded[3, :, 3 : basis_width + 6]
    )
    spilled = extended[:, basis_width:]
    arrived = passed_along(spilled, "tm", 1)
    proj = jnp.concatenate([extended[:, :3] + arrived, extended[:, 3:basis_width]], axis=1)
    total_basis = basis_width * lax.axis_size("tm")
    first_column = lax.axis_index("tm") * basis_width
    smooth_col = smoothing[:, None]
    margin = 2 * ITERS
    proj_wide = padded_2(proj, (("tm", 1),), margin)
    coefficients = proj_wide
    for sweep_number in range(ITERS):
        margin_now = margin - 2 * sweep_number
        index_wide = (
            first_column - margin_now + jnp.arange(basis_width + 2 * margin_now, dtype=jnp.int32)
        )
        offset = 2 * sweep_number + 2
        target = proj_wide[:, offset : offset + basis_width + 2 * margin_now - 4]
        coefficients = relax_sweep(coefficients, target, smooth_col, index_wide, total_basis)
    curve_total = row_count * lax.axis_size("curve")
    totals = lax.psum(jnp.sum(coefficients, axis=0), "curve")
    column_mean = totals / curve_total
    centered = coefficients - column_mean[None, :]
    partial_value = jnp.dot(
        centered, test_matrix, precision=lax.Precision.HIGHEST, preferred_element_type=jnp.float32
    )
    scores = lax.psum(partial_value, "tm")
    sketch_part = (
        jnp.einsum("ck,cr->kr", centered, scores, precision=lax.Precision.HIGHEST) / curve_total
    )
    owned_part = lax.psum_scatter(sketch_part, "curve", scatter_dimension=1, tiled=True)
    return (coefficients, scores, sketch_prev + owned_part)


def fits(mesh):
    groups = mesh.shape["curve"]
    return mesh.shape["tm"] == 2 and groups > 1 and groups & (groups - 1) == 0


def solution(mesh):
    placed = (P("curve", "tm"), P("curve"), P("tm", None), P("tm", "curve"))
    return jax.shard_map(
        fast_body if fits(mesh) else plain_body,
        mesh=mesh,
        in_specs=placed,
        out_specs=(P("curve", "tm"), P("curve", None), P("tm", "curve")),
        check_vma=False,
    )
```

```python
import functools

import jax
import jax.numpy as jnp
from jax import lax
from jax.experimental import pallas as pl
from jax.experimental.pallas import tpu as pltpu
from jax.sharding import PartitionSpec as P

SPB = 16
ITERS = 4
LANES = 128
TILE = LANES * SPB
CHUNK = 256
HEAD = 24
DEPTH = 5
WINDOW = HEAD + LANES
ZONE_LOW = 8
ZONE_HIGH = 16
EDGE = 24

RADIX_BITS = 2

damping = 0.45


def banded_weights():
    sample = lax.broadcasted_iota(jnp.int32, (CHUNK, LANES), 0)
    piece = lax.div(sample, SPB) + 3 - lax.broadcasted_iota(jnp.int32, (CHUNK, LANES), 1)
    frac = (lax.rem(sample, SPB).astype(jnp.float32) + 0.5) / SPB
    pieces = [
        frac**3 / 6.0,
        (-3.0 * frac**3 + 3.0 * frac**2 + 3.0 * frac + 1.0) / 6.0,
        (3.0 * frac**3 - 6.0 * frac**2 + 4.0) / 6.0,
        (1.0 - frac) ** 3 / 6.0,
    ]
    weights = jnp.zeros((CHUNK, LANES), jnp.float32)
    for which, value in enumerate(pieces):
        weights = jnp.where(piece == which, value / SPB, weights)
    return weights


def split_bf16(value):
    high = value.astype(jnp.bfloat16)
    return high, (value - high.astype(jnp.float32)).astype(jnp.bfloat16)


def dot32(a, b):
    return jnp.dot(a, b, preferred_element_type=jnp.float32)


def sweep_factors(smooth, diag):
    factor = damping / (1.0 + smooth * diag)
    pull = factor * smooth
    return 1.0 - factor - 6.0 * pull, 4.0 * pull, pull, factor


def relaxed(at_hand, near, far, target, factors):
    own, four, one, factor = factors
    return own * at_hand + factor * target + four * near - one * far


def curve_kernel(x_all, smooth_all, test_all, c_all, msg_ref, w_ref, main_ref, last_ref, proj_ref,
                 state_ref, done_ref, scored, strip_ref, x_ref, x_sems, test_ref, test_sem, c_ref, c_sems, smooth_ref, smooth_sem):
    rows, basis = c_all.shape
    blocks = basis // LANES
    rank = test_ref.shape[0]
    halves = rows // LANES
    height = WINDOW
    base = rank + EDGE
    has_left = lax.axis_index("tm") > 0
    has_right = lax.axis_index("tm") < lax.axis_size("tm") - 1
    sub = lax.broadcasted_iota(jnp.int32, (8, LANES), 0)

    def tile_at(which):
        return pl.ds(pl.multiple_of(which * LANES, LANES), LANES)

    def incoming(which):
        at = pl.ds(pl.multiple_of(which * TILE, TILE), TILE)
        slot = lax.rem(which, DEPTH)
        return pltpu.make_async_copy(x_all.at[:, at], x_ref.at[slot], x_sems.at[slot])

    def outgoing(which):
        at = tile_at(which)
        return pltpu.make_async_copy(c_ref.at[:, at], c_all.at[:, at], c_sems.at[which])

    def project(step, between):
        slot = lax.rem(step, 2)

        def chunk_dot(r):
            high, low = split_bf16(x_ref[lax.rem(step, DEPTH), :, r * CHUNK : (r + 1) * CHUNK])
            w = w_ref[r * CHUNK : (r + 1) * CHUNK, :]
            return dot32(high, w) + dot32(low, w)

        count = TILE // CHUNK
        for _ in between:
            pass
        rest = chunk_dot(count - 1)
        last_ref[slot] = rest[:, :LANES] + rest[:, LANES:]
        most = None
        for r in range(count - 1):
            part = chunk_dot(r)
            most = part if most is None else most + part
        for _ in between:
            pass
        main_ref[slot] = most[:, :LANES] + most[:, LANES:]

    def relax(block, is_end=False):
        slot, before = lax.rem(block + 2, 2), lax.rem(block + 1, 2)
        is_first = block == 0
        write_at = jnp.maximum(block, 0) * LANES
        for h in range(halves):
            cols = slice(h * LANES, (h + 1) * LANES)
            proj_ref[h, 8:HEAD, :] = proj_ref[h, LANES + 8 : LANES + HEAD, :]
            wide = lax.broadcasted_iota(jnp.int32, (LANES, LANES), 1)
            earlier = jnp.where(is_first, 0.0, last_ref[before, cols, :])
            here = main_ref[slot, cols, :] + jnp.where(wide < LANES // 2, earlier, last_ref[slot, cols, :])
            turned = here.T
            proj_ref[h, HEAD : HEAD + LANES, :] = turned
            if not is_end:
                strip_ref[h] = jnp.where(is_first, turned[:EDGE], strip_ref[h])
            else:
                spilled = last_ref[slot, cols, :].T[:8]
                ending = jnp.concatenate([turned[LANES - ZONE_HIGH :], spilled], axis=0)
                strip_ref[h] = jnp.where(has_right, ending, strip_ref[h])

            smooth = jnp.broadcast_to(smooth_ref[:, cols], (8, LANES))
            starting = closing = inner = sweep_factors(smooth, 6.0)
            if not is_end:
                diag = jnp.where(sub == 0, 1.0, jnp.where(sub == 1, 5.0, 6.0))
                starting = sweep_factors(smooth, jnp.where(is_first, diag, 6.0))
            else:
                closing = sweep_factors(smooth, jnp.where(sub == 7, 1.0, jnp.where(sub == 6, 5.0, 6.0)))

            def ghosts(ref, lead):
                def row(at):
                    return jnp.broadcast_to(ref[(*lead, slice(at, at + 1), slice(None))], (8, LANES))

                if not is_end:
                    zero, one = row(HEAD), row(HEAD + 1)
                    ahead = (*lead, slice(HEAD - 8, HEAD), slice(None))
                    outside = jnp.where(sub == 7, 2.0 * zero - one, 3.0 * zero - 2.0 * one)
                    ref[ahead] = jnp.where(is_first, outside, ref[ahead])
                else:
                    zero, one = row(height - 1), row(height - 2)
                    ref[(*lead, slice(height, height + 8), slice(None))] = jnp.where(
                        sub == 0, 2.0 * zero - one, 3.0 * zero - 2.0 * one
                    )

            ghosts(proj_ref, (h,))
            source, lead = proj_ref, (h,)
            for sweep in range(ITERS):
                final = sweep == ITERS - 1

                def load(at):
                    return source[(*lead, slice(at, at + 8), slice(None))]

                values = []
                for at in range(16 if final else 8, height, 8):
                    value = relaxed(
                        load(at),
                        load(at - 1) + load(at + 1),
                        load(at - 2) + load(at + 2),
                        proj_ref[h, at : at + 8, :],
                        starting if at == HEAD else closing if at == height - 8 else inner,
                    )
                    if final:
                        done_ref[h, pl.ds(pl.multiple_of(write_at + at - 16, 8), 8), :] = value
                    else:
                        state_ref[sweep, h, at : at + 8, :] = value
                if not final:
                    ghosts(state_ref, (sweep, h))
                    source, lead = state_ref, (sweep, h)
                yield

    def finish(which, end=False):
        parts = []
        for h in range(halves):
            where = pl.multiple_of(which * LANES + 8, 8)
            part = done_ref[h, pl.ds(where, LANES), :]
            c_ref[h * LANES : (h + 1) * LANES, tile_at(which)] = part.T
            parts.append(part)
        test = test_ref[:, tile_at(which)]
        wide = lax.broadcasted_iota(jnp.int32, (rank, LANES), 1)
        if not end:
            left_zone = jnp.logical_and(has_left, which == 0)
            test = jnp.where(jnp.logical_and(left_zone, wide < ZONE_HIGH), 0.0, test)
        else:
            test = jnp.where(jnp.logical_and(has_right, wide >= LANES - ZONE_LOW), 0.0, test)
        test_high, test_low = split_bf16(test)
        high, low = split_bf16(jnp.concatenate(parts, axis=1))
        both = dot32(jnp.concatenate([test_high, test_low], axis=0), high)
        more = both[:rank] + both[rank:] + dot32(test_high, low)
        scored[...] = jnp.where(which == 0, 0.0, scored[...]) + more

    smooth_copy = pltpu.make_async_copy(smooth_all, smooth_ref, smooth_sem)
    test_copy = pltpu.make_async_copy(test_all, test_ref, test_sem)
    smooth_copy.start()
    for which in range(min(DEPTH - 1, blocks)):
        incoming(which).start()
    test_copy.start()
    band = banded_weights()
    for r in range(TILE // CHUNK):
        high, low = split_bf16(pltpu.roll(band, r * (CHUNK // SPB), 1))
        w_ref[r * CHUNK : (r + 1) * CHUNK, :LANES] = high
        w_ref[r * CHUNK : (r + 1) * CHUNK, LANES:] = low
    smooth_copy.wait()

    def advance(step):
        @pl.when(step + DEPTH - 1 < blocks)
        def _():
            incoming(step + DEPTH - 1).start()

        incoming(step).wait()

    @pl.loop(0, 3)
    def _(step):
        advance(step)
        project(step, relax(step - 1))

    test_copy.wait()

    @pl.loop(3, blocks)
    def _(step):
        advance(step)
        finish(step - 3)
        project(step, relax(step - 1))
        outgoing(step - 3).start()

    finish(blocks - 3)
    outgoing(blocks - 3).start()
    for _ in relax(blocks - 1, is_end=True):
        pass
    finish(blocks - 2)
    outgoing(blocks - 2).start()
    finish(blocks - 1, end=True)
    outgoing(blocks - 1).start()

    msg_ref[:rank, :] = scored[...]
    for h in range(halves):
        msg_ref[rank:base, h * LANES : (h + 1) * LANES] = strip_ref[h]
    low_zone = padded_turn(test_ref[:, basis - LANES :])[LANES - ZONE_LOW :]
    high_zone = padded_turn(test_ref[:, :LANES])
    msg_ref[base:, :] = jnp.zeros_like(msg_ref[base:, :])
    msg_ref[base:, :LANES] = jnp.where(has_right, low_zone, high_zone[:8])
    msg_ref[base:, LANES : 2 * LANES] = high_zone[8:16]
    for which in range(blocks):
        outgoing(which).wait()


def padded_turn(part):
    fill = jnp.zeros((LANES - part.shape[0], LANES), part.dtype)
    return jnp.concatenate([part, fill], axis=0).T


def curve_stage(samples, smooth_row, test_t):
    rows, width = samples.shape
    rank, basis = test_t.shape
    blocks, halves = basis // LANES, rows // LANES
    f32, bf16 = jnp.float32, jnp.bfloat16
    vmem, hbm = pl.BlockSpec(memory_space=pltpu.VMEM), pl.BlockSpec(memory_space=pltpu.HBM)
    return pl.pallas_call(
        curve_kernel,
        out_shape=(
            jax.ShapeDtypeStruct((rows, basis), f32),
            jax.ShapeDtypeStruct((rank + EDGE + 8, rows), f32),
        ),
        in_specs=[hbm, hbm, hbm],
        out_specs=(hbm, vmem),
        scratch_shapes=[
            pltpu.VMEM((TILE, 2 * LANES), bf16),
            pltpu.VMEM((2, rows, LANES), f32),
            pltpu.VMEM((2, rows, LANES), f32),
            pltpu.VMEM((halves, WINDOW + 8, LANES), f32),
            pltpu.VMEM((ITERS - 1, halves, WINDOW + 8, LANES), f32),
            pltpu.VMEM((halves, basis + LANES, LANES), f32),
            pltpu.VMEM((rank, rows), f32),
            pltpu.VMEM((halves, EDGE, LANES), f32),
            pltpu.VMEM((DEPTH, rows, TILE), f32),
            pltpu.SemaphoreType.DMA((DEPTH,)),
            pltpu.VMEM((rank, basis), f32),
            pltpu.SemaphoreType.DMA,
            pltpu.VMEM((rows, basis), f32),
            pltpu.SemaphoreType.DMA((blocks,)),
            pltpu.VMEM((1, rows), f32),
            pltpu.SemaphoreType.DMA,
        ],
        compiler_params=pltpu.CompilerParams(
            vmem_limit_bytes=60 * 1024 * 1024,
        ),
        cost_estimate=pl.CostEstimate(
            flops=4 * rows * width * 2 * LANES, bytes_accessed=4 * rows * width, transcendentals=0
        ),
        name="curves",
    )(samples, smooth_row, test_t)


def relax_strip(strip, smooth_row):
    factor = damping / (1.0 + 6.0 * smooth_row)
    pull = factor * smooth_row
    height = strip.shape[0]
    pulled = factor * strip
    state = strip

    def difference(v):
        return pltpu.roll(v, 1, 0) + pltpu.roll(v, height - 1, 0) - (v + v)

    for _ in range(ITERS):
        state = (1.0 - factor) * state + pulled - pull * difference(difference(state))
    return state


def swapped(value, block, flip):
    parts = [value[at : at + block] for at in range(0, value.shape[0], block)]
    other = [parts[k ^ 1] for k in range(len(parts))]
    return jnp.where(flip, jnp.concatenate(other, axis=0), value)


def exchange_order(value, order, index):
    count = 1 << len(order)
    block = value.shape[0] // count
    owner = [sum(b for k, b in enumerate(order) if p >> (len(order) - 1 - k) & 1) for p in range(count)]
    value = jnp.concatenate([value[q * block : (q + 1) * block] for q in owner], axis=0)
    for k, bit in enumerate(order):
        value = swapped(value, value.shape[0] >> (k + 1), (index & bit) != 0)
    return value


def sketch_kernel(order, own_ref, own_edge_ref, came_ref, smooth_ref, c_in, c_ref, keep_ref, send_ref, total_ref,
                  c_all, tile_ref, load_sems, store_sem):
    rows, basis = c_in.shape
    rank = total_ref.shape[0]
    tiles = basis // LANES
    half = rank // 2
    has_left = lax.axis_index("tm") > 0
    parts = load_sems.shape[0]
    wide = basis // parts
    loads = []
    for k in range(parts):
        at = pl.ds(k * wide, wide)
        loads.append(pltpu.make_async_copy(c_in.at[:, at], c_all.at[:, at], load_sems.at[k]))
        loads[k].start()

    own, came = own_ref[...], came_ref[:rank, :]
    own_edge, came_edge = own_edge_ref[...], came_ref[rank:, :]
    low = jnp.where(has_left, came_edge, own_edge)
    high = jnp.where(has_left, own_edge, came_edge)
    fill = jnp.zeros((EDGE - ZONE_LOW, rows), jnp.float32)
    strip = jnp.concatenate([low[:EDGE], fill], axis=0) + jnp.concatenate([fill, high[:EDGE]], axis=0)
    fixed = relax_strip(strip, smooth_ref[...])[ZONE_LOW : ZONE_LOW + EDGE]
    zone_test = jnp.concatenate(
        [low[EDGE:, :LANES], high[EDGE:, :LANES], high[EDGE:, LANES : 2 * LANES]], axis=0
    )[:, :rank]
    zone_scores = lax.dot_general(
        zone_test, fixed, (((0,), (0,)), ((), ())),
        precision=lax.Precision.HIGHEST, preferred_element_type=jnp.float32,
    )
    total = own + came + zone_scores
    total_ref[...] = total

    placed = jnp.where(
        has_left,
        jnp.concatenate([fixed[ZONE_LOW:], jnp.zeros((LANES - ZONE_HIGH, rows), jnp.float32)], axis=0),
        jnp.concatenate([jnp.zeros((LANES - ZONE_LOW, rows), jnp.float32), fixed[:ZONE_LOW]], axis=0),
    )
    lane = lax.broadcasted_iota(jnp.int32, (LANES, LANES), 1)
    first, past = jnp.where(has_left, 0, LANES - ZONE_LOW), jnp.where(has_left, ZONE_HIGH, LANES)
    fix_lane = jnp.logical_and(lane >= first, lane < past)
    edge = pl.multiple_of(jnp.where(has_left, 0, basis - LANES), LANES)

    mean_score = jnp.mean(total, axis=1, keepdims=True)
    spread = jnp.broadcast_to(mean_score, (rank, LANES))
    score_row = padded_turn(spread)[:8]
    index = lax.axis_index("curve")
    spread = exchange_order(spread, order, index)
    lhs_high, lhs_low = split_bf16(exchange_order(total - mean_score, order, index))
    lhs = jnp.concatenate([lhs_high, lhs_low], axis=0)

    placed = [placed[:, at : at + LANES].T for at in range(0, rows, LANES)]
    placed = jnp.concatenate(placed, axis=0)
    fix_lane = jnp.concatenate([fix_lane.astype(jnp.int32)] * (rows // LANES), axis=0)
    store = pltpu.make_async_copy(tile_ref, c_ref.at[:, pl.ds(edge, LANES)], store_sem)

    for b in range(tiles):
        if b * LANES % wide == 0:
            loads[b * LANES // wide].wait()
        block = c_all[:, b * LANES : (b + 1) * LANES]
        if b in (0, tiles - 1):
            mine = has_left if b == 0 else jnp.logical_not(has_left)
            block = jnp.where(fix_lane * mine.astype(jnp.int32) > 0, placed, block)
            tile_ref[...] = block if b == 0 else jnp.where(has_left, tile_ref[...], block)
        mean = jnp.mean(block, axis=0, keepdims=True)
        rhs_high, rhs_low = split_bf16(block - mean)
        out = dot32(lhs, rhs_high)
        out = out[:rank] + out[rank:] + dot32(lhs_high, rhs_low)
        keep_ref[b * half : (b + 1) * half, :] = out[:half]
        send_ref[b * half : (b + 1) * half, :] = out[half:]
        at = (tiles + 1) * half + b
        keep_ref[at : at + 1, :] = mean
        send_ref[at : at + 1, :] = mean
    store.start()
    at = tiles * half
    keep_ref[at : at + half, :] = spread[:half]
    send_ref[at : at + half, :] = spread[half:]
    at = (tiles + 1) * half + tiles
    keep_ref[at:, :] = score_row
    send_ref[at:, :] = score_row
    store.wait()


def sketch_stage(message, came, smooth_row, coefficients, rank, order):
    rows, basis = coefficients.shape
    tiles = basis // LANES
    half = rank // 2
    f32 = jnp.float32
    packed = jax.ShapeDtypeStruct(((tiles + 1) * half + tiles + 8, LANES), f32)
    vmem, hbm = pl.BlockSpec(memory_space=pltpu.VMEM), pl.BlockSpec(memory_space=pltpu.HBM)
    return pl.pallas_call(
        functools.partial(sketch_kernel, order),
        out_shape=(
            jax.ShapeDtypeStruct((rows, basis), f32), packed, packed,
            jax.ShapeDtypeStruct((rank, rows), f32),
        ),
        in_specs=[vmem, vmem, vmem, vmem, hbm],
        out_specs=(hbm, vmem, vmem, vmem),
        scratch_shapes=[
            pltpu.VMEM((rows, basis), f32),
            pltpu.VMEM((rows, LANES), f32),
            pltpu.SemaphoreType.DMA((2,)),
            pltpu.SemaphoreType.DMA,
        ],
        input_output_aliases={4: 0},
        compiler_params=pltpu.CompilerParams(vmem_limit_bytes=16 * 1024 * 1024),
        cost_estimate=pl.CostEstimate(
            flops=6 * rows * basis * rank, bytes_accessed=4 * rows * basis, transcendentals=0
        ),
        name="sketch_part",
    )(message[:rank], message[rank:], came, smooth_row, coefficients)


def unpack(packed, tiles, height):
    moment = packed[: tiles * height].reshape(tiles, height, LANES)
    score = packed[tiles * height : (tiles + 1) * height]
    rest = packed[(tiles + 1) * height :]
    return moment, score, rest


def merged(one, other, count):
    moment, score, rest = one
    moment_2, score_2, rest_2 = other
    tiles = moment.shape[0]
    apart = rest[:tiles] - rest_2[:tiles]
    moment = moment + moment_2 + (0.5 * count) * apart[:, None, :] * (score - score_2)[None]
    return moment, 0.5 * (score + score_2), 0.5 * (rest + rest_2)


def packed_share(group, which, shares):
    moment, score, rest = group
    height = moment.shape[1] // shares
    part = slice(which * height, (which + 1) * height)
    return jnp.concatenate([moment[:, part].reshape(-1, LANES), score[part], rest], axis=0)


def exchanged(packed, groups, bits):
    return lax.ppermute(packed, "curve", [(i, i ^ bits) for i in range(groups)])


def fast_body(samples, smoothing, test_matrix, sketch_prev):
    rows, basis = samples.shape[0], test_matrix.shape[0]
    rank = test_matrix.shape[1]
    tiles = basis // LANES
    groups = lax.axis_size("curve")
    order = [1 << k for k in range(groups.bit_length() - 1)]
    smooth_row = smoothing[None, :]
    coefficients, message = curve_stage(samples, smooth_row, test_matrix.T)
    came = lax.ppermute(message, "tm", [(0, 1), (1, 0)])
    coefficients, keep, send, total = sketch_stage(message, came, smooth_row, coefficients, rank, order)
    height, count = rank // 2, rows
    came = exchanged(send, groups, order[0])
    group = merged(unpack(keep, tiles, height), unpack(came, tiles, height), count)
    count *= 2
    rest = order[1:]
    while rest:
        bits, rest = rest[:RADIX_BITS], rest[RADIX_BITS:]
        shares = 1 << len(bits)
        height //= shares
        parts = [unpack(packed_share(group, 0, shares), tiles, height)]
        for which in range(1, shares):
            partner = sum(b for k, b in enumerate(bits) if which >> (len(bits) - 1 - k) & 1)
            came = exchanged(packed_share(group, which, shares), groups, partner)
            parts.append(unpack(came, tiles, height))
        while len(parts) > 1:
            parts = [merged(parts[k], parts[k + 1], count) for k in range(0, len(parts), 2)]
            count *= 2
        group = parts[0]
    moment, _, rest = group
    score_mean = rest[tiles, :rank]
    scores = (total - score_mean[:, None]).T
    sketch = sketch_prev + moment.transpose(0, 2, 1).reshape(basis, height) / count
    return coefficients, scores, sketch


def passed_along(block, axis, distance):
    devices = range(lax.axis_size(axis))
    route = [(i - distance, i) for i in devices if i - distance in devices]
    return lax.ppermute(block, axis, route)


def padded_2(block, sides, width):
    for axis, dim in sides:
        count = lax.axis_size(axis)
        forward = [(i, i + 1) for i in range(count - 1)]
        backward = [(target, source) for source, target in forward]
        low = lax.ppermute(
            lax.slice_in_dim(block, block.shape[dim] - width, None, axis=dim), axis, forward
        )
        high = lax.ppermute(lax.slice_in_dim(block, 0, width, axis=dim), axis, backward)
        block = jnp.concatenate([low, block, high], axis=dim)
    return block


def weight_table():
    frac = (jnp.arange(SPB, dtype=jnp.float32) + 0.5) / SPB
    pieces = [
        frac**3 / 6.0,
        (-3.0 * frac**3 + 3.0 * frac**2 + 3.0 * frac + 1.0) / 6.0,
        (3.0 * frac**3 - 6.0 * frac**2 + 4.0) / 6.0,
        (1.0 - frac) ** 3 / 6.0,
    ]
    return jnp.stack(pieces) / SPB


def relax_sweep(widened, target, smooth_col, index_wide, total_basis):
    second = widened[:, 2:] - 2.0 * widened[:, 1:-1] + widened[:, :-2]
    in_range = (index_wide[:-2] >= 0) & (index_wide[:-2] <= total_basis - 3)
    second = jnp.where(in_range[None, :], second, 0.0)
    bending = second[:, 2:] - 2.0 * second[:, 1:-1] + second[:, :-2]
    interior = widened[:, 2:-2]
    column_index = index_wide[2:-2]
    penalty_diag = (
        (column_index <= total_basis - 3).astype(jnp.float32)
        + 4.0 * ((column_index >= 1) & (column_index <= total_basis - 2)).astype(jnp.float32)
        + (column_index >= 2).astype(jnp.float32)
    )
    return interior + damping * (target - interior - smooth_col * bending) / (
        1.0 + smooth_col * penalty_diag
    )


def plain_body(samples, smoothing, test_matrix, sketch_prev):
    row_count = samples.shape[0]
    basis_width = samples.shape[1] // SPB
    blocks = samples.reshape(row_count, basis_width, SPB)
    segment_sums = jnp.einsum(
        "cgq,mq->mcg", blocks, weight_table(), precision=lax.Precision.HIGHEST
    )
    padded = jnp.pad(segment_sums, ((0, 0), (0, 0), (3, 3)))
    extended = (
        padded[0, :, 0 : basis_width + 3]
        + padded[1, :, 1 : basis_width + 4]
        + padded[2, :, 2 : basis_width + 5]
        + padded[3, :, 3 : basis_width + 6]
    )
    spilled = extended[:, basis_width:]
    arrived = passed_along(spilled, "tm", 1)
    proj = jnp.concatenate([extended[:, :3] + arrived, extended[:, 3:basis_width]], axis=1)
    total_basis = basis_width * lax.axis_size("tm")
    first_column = lax.axis_index("tm") * basis_width
    smooth_col = smoothing[:, None]
    margin = 2 * ITERS
    proj_wide = padded_2(proj, (("tm", 1),), margin)
    coefficients = proj_wide
    for sweep_number in range(ITERS):
        margin_now = margin - 2 * sweep_number
        index_wide = (
            first_column - margin_now + jnp.arange(basis_width + 2 * margin_now, dtype=jnp.int32)
        )
        offset = 2 * sweep_number + 2
        target = proj_wide[:, offset : offset + basis_width + 2 * margin_now - 4]
        coefficients = relax_sweep(coefficients, target, smooth_col, index_wide, total_basis)
    curve_total = row_count * lax.axis_size("curve")
    totals = lax.psum(jnp.sum(coefficients, axis=0), "curve")
    column_mean = totals / curve_total
    centered = coefficients - column_mean[None, :]
    partial_value = jnp.dot(
        centered, test_matrix, precision=lax.Precision.HIGHEST, preferred_element_type=jnp.float32
    )
    scores = lax.psum(partial_value, "tm")
    sketch_part = (
        jnp.einsum("ck,cr->kr", centered, scores, precision=lax.Precision.HIGHEST) / curve_total
    )
    owned_part = lax.psum_scatter(sketch_part, "curve", scatter_dimension=1, tiled=True)
    return (coefficients, scores, sketch_prev + owned_part)


def fits(mesh):
    groups = mesh.shape["curve"]
    return mesh.shape["tm"] == 2 and groups > 1 and groups & (groups - 1) == 0


def solution(mesh):
    placed = (P("curve", "tm"), P("curve"), P("tm", None), P("tm", "curve"))
    return jax.shard_map(
        fast_body if fits(mesh) else plain_body,
        mesh=mesh,
        in_specs=placed,
        out_specs=(P("curve", "tm"), P("curve", None), P("tm", "curve")),
        check_vma=False,
    )
```

```python
import functools

import jax
import jax.numpy as jnp
from jax import lax
from jax.experimental import pallas as pl
from jax.experimental.pallas import tpu as pltpu
from jax.sharding import PartitionSpec as P

SPB = 16
ITERS = 4
LANES = 128
TILE = LANES * SPB
CHUNK = 256
HEAD = 24
DEPTH = 5
WINDOW = HEAD + LANES
ZONE_LOW = 8
ZONE_HIGH = 16
EDGE = 24

RADIX_BITS = 2

damping = 0.45


def banded_weights():
    sample = lax.broadcasted_iota(jnp.int32, (CHUNK, LANES), 0)
    piece = lax.div(sample, SPB) + 3 - lax.broadcasted_iota(jnp.int32, (CHUNK, LANES), 1)
    frac = (lax.rem(sample, SPB).astype(jnp.float32) + 0.5) / SPB
    pieces = [
        frac**3 / 6.0,
        (-3.0 * frac**3 + 3.0 * frac**2 + 3.0 * frac + 1.0) / 6.0,
        (3.0 * frac**3 - 6.0 * frac**2 + 4.0) / 6.0,
        (1.0 - frac) ** 3 / 6.0,
    ]
    weights = jnp.zeros((CHUNK, LANES), jnp.float32)
    for which, value in enumerate(pieces):
        weights = jnp.where(piece == which, value / SPB, weights)
    return weights


def split_bf16(value):
    high = value.astype(jnp.bfloat16)
    return high, (value - high.astype(jnp.float32)).astype(jnp.bfloat16)


def dot32(a, b):
    return jnp.dot(a, b, preferred_element_type=jnp.float32)


def sweep_factors(smooth, diag):
    factor = damping / (1.0 + smooth * diag)
    pull = factor * smooth
    return 1.0 - factor - 6.0 * pull, 4.0 * pull, pull, factor


def relaxed(at_hand, near, far, target, factors):
    own, four, one, factor = factors
    return own * at_hand + factor * target + four * near - one * far


def curve_kernel(x_all, smooth_all, test_all, c_all, msg_ref, w_ref, main_ref, last_ref, proj_ref,
                 state_ref, done_ref, scored, strip_ref, x_ref, x_sems, test_ref, test_sem, c_ref, c_sems, smooth_ref, smooth_sem):
    rows, basis = c_all.shape
    blocks = basis // LANES
    rank = test_ref.shape[0]
    halves = rows // LANES
    height = WINDOW
    base = rank + EDGE
    has_left = lax.axis_index("tm") > 0
    has_right = lax.axis_index("tm") < lax.axis_size("tm") - 1
    sub = lax.broadcasted_iota(jnp.int32, (8, LANES), 0)

    def tile_at(which):
        return pl.ds(pl.multiple_of(which * LANES, LANES), LANES)

    def incoming(which):
        at = pl.ds(pl.multiple_of(which * TILE, TILE), TILE)
        slot = lax.rem(which, DEPTH)
        return pltpu.make_async_copy(x_all.at[:, at], x_ref.at[slot], x_sems.at[slot])

    def outgoing(which):
        at = tile_at(which)
        return pltpu.make_async_copy(c_ref.at[:, at], c_all.at[:, at], c_sems.at[which])

    def project(step, between):
        slot = lax.rem(step, 2)

        def chunk_dot(r):
            high, low = split_bf16(x_ref[lax.rem(step, DEPTH), :, r * CHUNK : (r + 1) * CHUNK])
            w = w_ref[r * CHUNK : (r + 1) * CHUNK, :]
            return dot32(high, w) + dot32(low, w)

        count = TILE // CHUNK
        for _ in between:
            pass
        rest = chunk_dot(count - 1)
        last_ref[slot] = rest[:, :LANES] + rest[:, LANES:]
        most = None
        for r in range(count - 1):
            part = chunk_dot(r)
            most = part if most is None else most + part
        for _ in between:
            pass
        main_ref[slot] = most[:, :LANES] + most[:, LANES:]

    def relax(block, is_end=False):
        slot, before = lax.rem(block + 2, 2), lax.rem(block + 1, 2)
        is_first = block == 0
        write_at = jnp.maximum(block, 0) * LANES
        for h in range(halves):
            cols = slice(h * LANES, (h + 1) * LANES)
            proj_ref[h, 8:HEAD, :] = proj_ref[h, LANES + 8 : LANES + HEAD, :]
            wide = lax.broadcasted_iota(jnp.int32, (LANES, LANES), 1)
            earlier = jnp.where(is_first, 0.0, last_ref[before, cols, :])
            here = main_ref[slot, cols, :] + jnp.where(wide < LANES // 2, earlier, last_ref[slot, cols, :])
            turned = here.T
            proj_ref[h, HEAD : HEAD + LANES, :] = turned
            if not is_end:
                strip_ref[h] = jnp.where(is_first, turned[:EDGE], strip_ref[h])
            else:
                spilled = last_ref[slot, cols, :].T[:8]
                ending = jnp.concatenate([turned[LANES - ZONE_HIGH :], spilled], axis=0)
                strip_ref[h] = jnp.where(has_right, ending, strip_ref[h])

            smooth = jnp.broadcast_to(smooth_ref[:, cols], (8, LANES))
            starting = closing = inner = sweep_factors(smooth, 6.0)
            if not is_end:
                diag = jnp.where(sub == 0, 1.0, jnp.where(sub == 1, 5.0, 6.0))
                starting = sweep_factors(smooth, jnp.where(is_first, diag, 6.0))
            else:
                closing = sweep_factors(smooth, jnp.where(sub == 7, 1.0, jnp.where(sub == 6, 5.0, 6.0)))

            def ghosts(ref, lead):
                def row(at):
                    return jnp.broadcast_to(ref[(*lead, slice(at, at + 1), slice(None))], (8, LANES))

                if not is_end:
                    zero, one = row(HEAD), row(HEAD + 1)
                    ahead = (*lead, slice(HEAD - 8, HEAD), slice(None))
                    outside = jnp.where(sub == 7, 2.0 * zero - one, 3.0 * zero - 2.0 * one)
                    ref[ahead] = jnp.where(is_first, outside, ref[ahead])
                else:
                    zero, one = row(height - 1), row(height - 2)
                    ref[(*lead, slice(height, height + 8), slice(None))] = jnp.where(
                        sub == 0, 2.0 * zero - one, 3.0 * zero - 2.0 * one
                    )

            ghosts(proj_ref, (h,))
            source, lead = proj_ref, (h,)
            for sweep in range(ITERS):
                final = sweep == ITERS - 1

                def load(at):
                    return source[(*lead, slice(at, at + 8), slice(None))]

                values = []
                for at in range(16 if final else 8, height, 8):
                    value = relaxed(
                        load(at),
                        load(at - 1) + load(at + 1),
                        load(at - 2) + load(at + 2),
                        proj_ref[h, at : at + 8, :],
                        starting if at == HEAD else closing if at == height - 8 else inner,
                    )
                    if final:
                        done_ref[h, pl.ds(pl.multiple_of(write_at + at - 16, 8), 8), :] = value
                    else:
                        state_ref[sweep, h, at : at + 8, :] = value
                if not final:
                    ghosts(state_ref, (sweep, h))
                    source, lead = state_ref, (sweep, h)
                yield

    def finish(which, end=False):
        parts = []
        for h in range(halves):
            where = pl.multiple_of(which * LANES + 8, 8)
            part = done_ref[h, pl.ds(where, LANES), :]
            c_ref[h * LANES : (h + 1) * LANES, tile_at(which)] = part.T
            parts.append(part)
        test = test_ref[:, tile_at(which)]
        wide = lax.broadcasted_iota(jnp.int32, (rank, LANES), 1)
        if not end:
            left_zone = jnp.logical_and(has_left, which == 0)
            test = jnp.where(jnp.logical_and(left_zone, wide < ZONE_HIGH), 0.0, test)
        else:
            test = jnp.where(jnp.logical_and(has_right, wide >= LANES - ZONE_LOW), 0.0, test)
        test_high, test_low = split_bf16(test)
        high, low = split_bf16(jnp.concatenate(parts, axis=1))
        both = dot32(jnp.concatenate([test_high, test_low], axis=0), high)
        more = both[:rank] + both[rank:] + dot32(test_high, low)
        scored[...] = jnp.where(which == 0, 0.0, scored[...]) + more

    smooth_copy = pltpu.make_async_copy(smooth_all, smooth_ref, smooth_sem)
    test_copy = pltpu.make_async_copy(test_all, test_ref, test_sem)
    smooth_copy.start()
    for which in range(min(DEPTH - 1, blocks)):
        incoming(which).start()
    test_copy.start()
    band = banded_weights()
    for r in range(TILE // CHUNK):
        high, low = split_bf16(pltpu.roll(band, r * (CHUNK // SPB), 1))
        w_ref[r * CHUNK : (r + 1) * CHUNK, :LANES] = high
        w_ref[r * CHUNK : (r + 1) * CHUNK, LANES:] = low
    smooth_copy.wait()

    def advance(step):
        @pl.when(step + DEPTH - 1 < blocks)
        def _():
            incoming(step + DEPTH - 1).start()

        incoming(step).wait()

    @pl.loop(0, 3)
    def _(step):
        advance(step)
        project(step, relax(step - 1))

    test_copy.wait()

    @pl.loop(3, blocks)
    def _(step):
        advance(step)
        finish(step - 3)
        project(step, relax(step - 1))
        outgoing(step - 3).start()

    finish(blocks - 3)
    outgoing(blocks - 3).start()
    for _ in relax(blocks - 1, is_end=True):
        pass
    finish(blocks - 2)
    outgoing(blocks - 2).start()
    finish(blocks - 1, end=True)
    outgoing(blocks - 1).start()

    msg_ref[:rank, :] = scored[...]
    for h in range(halves):
        msg_ref[rank:base, h * LANES : (h + 1) * LANES] = strip_ref[h]
    low_zone = padded_turn(test_ref[:, basis - LANES :])[LANES - ZONE_LOW :]
    high_zone = padded_turn(test_ref[:, :LANES])
    msg_ref[base:, :] = jnp.zeros_like(msg_ref[base:, :])
    msg_ref[base:, :LANES] = jnp.where(has_right, low_zone, high_zone[:8])
    msg_ref[base:, LANES : 2 * LANES] = high_zone[8:16]
    for which in range(blocks):
        outgoing(which).wait()


def padded_turn(part):
    fill = jnp.zeros((LANES - part.shape[0], LANES), part.dtype)
    return jnp.concatenate([part, fill], axis=0).T


def curve_stage(samples, smooth_row, test_t):
    rows, width = samples.shape
    rank, basis = test_t.shape
    blocks, halves = basis // LANES, rows // LANES
    f32, bf16 = jnp.float32, jnp.bfloat16
    vmem, hbm = pl.BlockSpec(memory_space=pltpu.VMEM), pl.BlockSpec(memory_space=pltpu.HBM)
    return pl.pallas_call(
        curve_kernel,
        out_shape=(
            jax.ShapeDtypeStruct((rows, basis), f32),
            jax.ShapeDtypeStruct((rank + EDGE + 8, rows), f32),
        ),
        in_specs=[hbm, hbm, hbm],
        out_specs=(hbm, vmem),
        scratch_shapes=[
            pltpu.VMEM((TILE, 2 * LANES), bf16),
            pltpu.VMEM((2, rows, LANES), f32),
            pltpu.VMEM((2, rows, LANES), f32),
            pltpu.VMEM((halves, WINDOW + 8, LANES), f32),
            pltpu.VMEM((ITERS - 1, halves, WINDOW + 8, LANES), f32),
            pltpu.VMEM((halves, basis + LANES, LANES), f32),
            pltpu.VMEM((rank, rows), f32),
            pltpu.VMEM((halves, EDGE, LANES), f32),
            pltpu.VMEM((DEPTH, rows, TILE), f32),
            pltpu.SemaphoreType.DMA((DEPTH,)),
            pltpu.VMEM((rank, basis), f32),
            pltpu.SemaphoreType.DMA,
            pltpu.VMEM((rows, basis), f32),
            pltpu.SemaphoreType.DMA((blocks,)),
            pltpu.VMEM((1, rows), f32),
            pltpu.SemaphoreType.DMA,
        ],
        compiler_params=pltpu.CompilerParams(
            vmem_limit_bytes=60 * 1024 * 1024,
        ),
        cost_estimate=pl.CostEstimate(
            flops=4 * rows * width * 2 * LANES, bytes_accessed=4 * rows * width, transcendentals=0
        ),
        name="curves",
    )(samples, smooth_row, test_t)


def relax_strip(strip, smooth_row):
    factor = damping / (1.0 + 6.0 * smooth_row)
    pull = factor * smooth_row
    height = strip.shape[0]
    pulled = factor * strip
    state = strip

    def difference(v):
        return pltpu.roll(v, 1, 0) + pltpu.roll(v, height - 1, 0) - (v + v)

    for _ in range(ITERS):
        state = (1.0 - factor) * state + pulled - pull * difference(difference(state))
    return state


def swapped(value, block, flip):
    parts = [value[at : at + block] for at in range(0, value.shape[0], block)]
    other = [parts[k ^ 1] for k in range(len(parts))]
    return jnp.where(flip, jnp.concatenate(other, axis=0), value)


def exchange_order(value, order, index):
    count = 1 << len(order)
    block = value.shape[0] // count
    owner = [sum(b for k, b in enumerate(order) if p >> (len(order) - 1 - k) & 1) for p in range(count)]
    value = jnp.concatenate([value[q * block : (q + 1) * block] for q in owner], axis=0)
    for k, bit in enumerate(order):
        value = swapped(value, value.shape[0] >> (k + 1), (index & bit) != 0)
    return value


def sketch_kernel(order, own_ref, own_edge_ref, came_ref, smooth_ref, c_low, c_high, c_in, c_ref, keep_ref,
                  send_ref, total_ref, tile_ref, store_sem):
    rows, basis = c_in.shape
    wide = basis // 2
    rank = total_ref.shape[0]
    tiles = basis // LANES
    half = rank // 2
    has_left = lax.axis_index("tm") > 0
    own, came = own_ref[...], came_ref[:rank, :]
    own_edge, came_edge = own_edge_ref[...], came_ref[rank:, :]
    low = jnp.where(has_left, came_edge, own_edge)
    high = jnp.where(has_left, own_edge, came_edge)
    fill = jnp.zeros((EDGE - ZONE_LOW, rows), jnp.float32)
    strip = jnp.concatenate([low[:EDGE], fill], axis=0) + jnp.concatenate([fill, high[:EDGE]], axis=0)
    fixed = relax_strip(strip, smooth_ref[...])[ZONE_LOW : ZONE_LOW + EDGE]
    zone_test = jnp.concatenate(
        [low[EDGE:, :LANES], high[EDGE:, :LANES], high[EDGE:, LANES : 2 * LANES]], axis=0
    )[:, :rank]
    zone_scores = lax.dot_general(
        zone_test, fixed, (((0,), (0,)), ((), ())),
        precision=lax.Precision.HIGHEST, preferred_element_type=jnp.float32,
    )
    total = own + came + zone_scores
    total_ref[...] = total

    placed = jnp.where(
        has_left,
        jnp.concatenate([fixed[ZONE_LOW:], jnp.zeros((LANES - ZONE_HIGH, rows), jnp.float32)], axis=0),
        jnp.concatenate([jnp.zeros((LANES - ZONE_LOW, rows), jnp.float32), fixed[:ZONE_LOW]], axis=0),
    )
    lane = lax.broadcasted_iota(jnp.int32, (LANES, LANES), 1)
    first, past = jnp.where(has_left, 0, LANES - ZONE_LOW), jnp.where(has_left, ZONE_HIGH, LANES)
    fix_lane = jnp.logical_and(lane >= first, lane < past)
    edge = pl.multiple_of(jnp.where(has_left, 0, basis - LANES), LANES)

    mean_score = jnp.mean(total, axis=1, keepdims=True)
    spread = jnp.broadcast_to(mean_score, (rank, LANES))
    score_row = padded_turn(spread)[:8]
    index = lax.axis_index("curve")
    spread = exchange_order(spread, order, index)
    lhs_high, lhs_low = split_bf16(exchange_order(total - mean_score, order, index))
    lhs = jnp.concatenate([lhs_high, lhs_low], axis=0)

    placed = [placed[:, at : at + LANES].T for at in range(0, rows, LANES)]
    placed = jnp.concatenate(placed, axis=0)
    fix_lane = jnp.concatenate([fix_lane.astype(jnp.int32)] * (rows // LANES), axis=0)
    store = pltpu.make_async_copy(tile_ref, c_ref.at[:, pl.ds(edge, LANES)], store_sem)

    for b in range(tiles):
        part, at = (c_low, b * LANES) if b * LANES < wide else (c_high, b * LANES - wide)
        block = part[:, at : at + LANES]
        if b in (0, tiles - 1):
            mine = has_left if b == 0 else jnp.logical_not(has_left)
            block = jnp.where(fix_lane * mine.astype(jnp.int32) > 0, placed, block)
            tile_ref[...] = block if b == 0 else jnp.where(has_left, tile_ref[...], block)
        mean = jnp.mean(block, axis=0, keepdims=True)
        rhs_high, rhs_low = split_bf16(block - mean)
        out = dot32(lhs, rhs_high)
        out = out[:rank] + out[rank:] + dot32(lhs_high, rhs_low)
        keep_ref[b * half : (b + 1) * half, :] = out[:half]
        send_ref[b * half : (b + 1) * half, :] = out[half:]
        at = (tiles + 1) * half + b
        keep_ref[at : at + 1, :] = mean
        send_ref[at : at + 1, :] = mean
    store.start()
    at = tiles * half
    keep_ref[at : at + half, :] = spread[:half]
    send_ref[at : at + half, :] = spread[half:]
    at = (tiles + 1) * half + tiles
    keep_ref[at:, :] = score_row
    send_ref[at:, :] = score_row
    store.wait()


def sketch_stage(message, came, smooth_row, coefficients, rank, order):
    rows, basis = coefficients.shape
    tiles = basis // LANES
    half = rank // 2
    f32 = jnp.float32
    packed = jax.ShapeDtypeStruct(((tiles + 1) * half + tiles + 8, LANES), f32)
    vmem, hbm = pl.BlockSpec(memory_space=pltpu.VMEM), pl.BlockSpec(memory_space=pltpu.HBM)
    return pl.pallas_call(
        functools.partial(sketch_kernel, order),
        out_shape=(
            jax.ShapeDtypeStruct((rows, basis), f32), packed, packed,
            jax.ShapeDtypeStruct((rank, rows), f32),
        ),
        in_specs=[vmem] * 6 + [hbm],
        out_specs=(hbm, vmem, vmem, vmem),
        scratch_shapes=[
            pltpu.VMEM((rows, LANES), f32),
            pltpu.SemaphoreType.DMA,
        ],
        input_output_aliases={6: 0},
        compiler_params=pltpu.CompilerParams(vmem_limit_bytes=16 * 1024 * 1024),
        cost_estimate=pl.CostEstimate(
            flops=6 * rows * basis * rank, bytes_accessed=4 * rows * basis, transcendentals=0
        ),
        name="sketch_part",
    )(
        message[:rank], message[rank:], came, smooth_row,
        coefficients[:, : basis // 2], coefficients[:, basis // 2 :], coefficients,
    )


def unpack(packed, tiles, height):
    moment = packed[: tiles * height].reshape(tiles, height, LANES)
    score = packed[tiles * height : (tiles + 1) * height]
    rest = packed[(tiles + 1) * height :]
    return moment, score, rest


def merged(one, other, count):
    moment, score, rest = one
    moment_2, score_2, rest_2 = other
    tiles = moment.shape[0]
    apart = rest[:tiles] - rest_2[:tiles]
    moment = moment + moment_2 + (0.5 * count) * apart[:, None, :] * (score - score_2)[None]
    return moment, 0.5 * (score + score_2), 0.5 * (rest + rest_2)


def packed_share(group, which, shares):
    moment, score, rest = group
    height = moment.shape[1] // shares
    part = slice(which * height, (which + 1) * height)
    return jnp.concatenate([moment[:, part].reshape(-1, LANES), score[part], rest], axis=0)


def exchanged(packed, groups, bits):
    return lax.ppermute(packed, "curve", [(i, i ^ bits) for i in range(groups)])


def fast_body(samples, smoothing, test_matrix, sketch_prev):
    rows, basis = samples.shape[0], test_matrix.shape[0]
    rank = test_matrix.shape[1]
    tiles = basis // LANES
    groups = lax.axis_size("curve")
    order = [1 << k for k in range(groups.bit_length() - 1)]
    smooth_row = smoothing[None, :]
    coefficients, message = curve_stage(samples, smooth_row, test_matrix.T)
    came = lax.ppermute(message, "tm", [(0, 1), (1, 0)])
    coefficients, keep, send, total = sketch_stage(message, came, smooth_row, coefficients, rank, order)
    height, count = rank // 2, rows
    came = exchanged(send, groups, order[0])
    group = merged(unpack(keep, tiles, height), unpack(came, tiles, height), count)
    count *= 2
    rest = order[1:]
    while rest:
        bits, rest = rest[:RADIX_BITS], rest[RADIX_BITS:]
        shares = 1 << len(bits)
        height //= shares
        parts = [unpack(packed_share(group, 0, shares), tiles, height)]
        for which in range(1, shares):
            partner = sum(b for k, b in enumerate(bits) if which >> (len(bits) - 1 - k) & 1)
            came = exchanged(packed_share(group, which, shares), groups, partner)
            parts.append(unpack(came, tiles, height))
        while len(parts) > 1:
            parts = [merged(parts[k], parts[k + 1], count) for k in range(0, len(parts), 2)]
            count *= 2
        group = parts[0]
    moment, _, rest = group
    score_mean = rest[tiles, :rank]
    scores = (total - score_mean[:, None]).T
    sketch = sketch_prev + moment.transpose(0, 2, 1).reshape(basis, height) / count
    return coefficients, scores, sketch


def passed_along(block, axis, distance):
    devices = range(lax.axis_size(axis))
    route = [(i - distance, i) for i in devices if i - distance in devices]
    return lax.ppermute(block, axis, route)


def padded_2(block, sides, width):
    for axis, dim in sides:
        count = lax.axis_size(axis)
        forward = [(i, i + 1) for i in range(count - 1)]
        backward = [(target, source) for source, target in forward]
        low = lax.ppermute(
            lax.slice_in_dim(block, block.shape[dim] - width, None, axis=dim), axis, forward
        )
        high = lax.ppermute(lax.slice_in_dim(block, 0, width, axis=dim), axis, backward)
        block = jnp.concatenate([low, block, high], axis=dim)
    return block


def weight_table():
    frac = (jnp.arange(SPB, dtype=jnp.float32) + 0.5) / SPB
    pieces = [
        frac**3 / 6.0,
        (-3.0 * frac**3 + 3.0 * frac**2 + 3.0 * frac + 1.0) / 6.0,
        (3.0 * frac**3 - 6.0 * frac**2 + 4.0) / 6.0,
        (1.0 - frac) ** 3 / 6.0,
    ]
    return jnp.stack(pieces) / SPB


def relax_sweep(widened, target, smooth_col, index_wide, total_basis):
    second = widened[:, 2:] - 2.0 * widened[:, 1:-1] + widened[:, :-2]
    in_range = (index_wide[:-2] >= 0) & (index_wide[:-2] <= total_basis - 3)
    second = jnp.where(in_range[None, :], second, 0.0)
    bending = second[:, 2:] - 2.0 * second[:, 1:-1] + second[:, :-2]
    interior = widened[:, 2:-2]
    column_index = index_wide[2:-2]
    penalty_diag = (
        (column_index <= total_basis - 3).astype(jnp.float32)
        + 4.0 * ((column_index >= 1) & (column_index <= total_basis - 2)).astype(jnp.float32)
        + (column_index >= 2).astype(jnp.float32)
    )
    return interior + damping * (target - interior - smooth_col * bending) / (
        1.0 + smooth_col * penalty_diag
    )


def plain_body(samples, smoothing, test_matrix, sketch_prev):
    row_count = samples.shape[0]
    basis_width = samples.shape[1] // SPB
    blocks = samples.reshape(row_count, basis_width, SPB)
    segment_sums = jnp.einsum(
        "cgq,mq->mcg", blocks, weight_table(), precision=lax.Precision.HIGHEST
    )
    padded = jnp.pad(segment_sums, ((0, 0), (0, 0), (3, 3)))
    extended = (
        padded[0, :, 0 : basis_width + 3]
        + padded[1, :, 1 : basis_width + 4]
        + padded[2, :, 2 : basis_width + 5]
        + padded[3, :, 3 : basis_width + 6]
    )
    spilled = extended[:, basis_width:]
    arrived = passed_along(spilled, "tm", 1)
    proj = jnp.concatenate([extended[:, :3] + arrived, extended[:, 3:basis_width]], axis=1)
    total_basis = basis_width * lax.axis_size("tm")
    first_column = lax.axis_index("tm") * basis_width
    smooth_col = smoothing[:, None]
    margin = 2 * ITERS
    proj_wide = padded_2(proj, (("tm", 1),), margin)
    coefficients = proj_wide
    for sweep_number in range(ITERS):
        margin_now = margin - 2 * sweep_number
        index_wide = (
            first_column - margin_now + jnp.arange(basis_width + 2 * margin_now, dtype=jnp.int32)
        )
        offset = 2 * sweep_number + 2
        target = proj_wide[:, offset : offset + basis_width + 2 * margin_now - 4]
        coefficients = relax_sweep(coefficients, target, smooth_col, index_wide, total_basis)
    curve_total = row_count * lax.axis_size("curve")
    totals = lax.psum(jnp.sum(coefficients, axis=0), "curve")
    column_mean = totals / curve_total
    centered = coefficients - column_mean[None, :]
    partial_value = jnp.dot(
        centered, test_matrix, precision=lax.Precision.HIGHEST, preferred_element_type=jnp.float32
    )
    scores = lax.psum(partial_value, "tm")
    sketch_part = (
        jnp.einsum("ck,cr->kr", centered, scores, precision=lax.Precision.HIGHEST) / curve_total
    )
    owned_part = lax.psum_scatter(sketch_part, "curve", scatter_dimension=1, tiled=True)
    return (coefficients, scores, sketch_prev + owned_part)


def fits(mesh):
    groups = mesh.shape["curve"]
    return mesh.shape["tm"] == 2 and groups > 1 and groups & (groups - 1) == 0


def solution(mesh):
    placed = (P("curve", "tm"), P("curve"), P("tm", None), P("tm", "curve"))
    return jax.shard_map(
        fast_body if fits(mesh) else plain_body,
        mesh=mesh,
        in_specs=placed,
        out_specs=(P("curve", "tm"), P("curve", None), P("tm", "curve")),
        check_vma=False,
    )
```

```python
import functools

import jax
import jax.numpy as jnp
from jax import lax
from jax.experimental import pallas as pl
from jax.experimental.pallas import tpu as pltpu
from jax.sharding import PartitionSpec as P

SPB = 16
ITERS = 4
LANES = 128
TILE = LANES * SPB
CHUNK = 256
HEAD = 24
DEPTH = 5
WINDOW = HEAD + LANES
ZONE_LOW = 8
ZONE_HIGH = 16
EDGE = 24

RADIX_BITS = 3

damping = 0.45


def banded_weights():
    sample = lax.broadcasted_iota(jnp.int32, (CHUNK, LANES), 0)
    piece = lax.div(sample, SPB) + 3 - lax.broadcasted_iota(jnp.int32, (CHUNK, LANES), 1)
    frac = (lax.rem(sample, SPB).astype(jnp.float32) + 0.5) / SPB
    pieces = [
        frac**3 / 6.0,
        (-3.0 * frac**3 + 3.0 * frac**2 + 3.0 * frac + 1.0) / 6.0,
        (3.0 * frac**3 - 6.0 * frac**2 + 4.0) / 6.0,
        (1.0 - frac) ** 3 / 6.0,
    ]
    weights = jnp.zeros((CHUNK, LANES), jnp.float32)
    for which, value in enumerate(pieces):
        weights = jnp.where(piece == which, value / SPB, weights)
    return weights


def split_bf16(value):
    high = value.astype(jnp.bfloat16)
    return high, (value - high.astype(jnp.float32)).astype(jnp.bfloat16)


def dot32(a, b):
    return jnp.dot(a, b, preferred_element_type=jnp.float32)


def sweep_factors(smooth, diag):
    factor = damping / (1.0 + smooth * diag)
    pull = factor * smooth
    return 1.0 - factor - 6.0 * pull, 4.0 * pull, pull, factor


def relaxed(at_hand, near, far, target, factors):
    own, four, one, factor = factors
    return own * at_hand + factor * target + four * near - one * far


def curve_kernel(x_all, smooth_all, test_all, c_all, msg_ref, w_ref, main_ref, last_ref, proj_ref,
                 state_ref, done_ref, scored, strip_ref, x_ref, x_sems, test_ref, test_sem, c_ref, c_sems, smooth_ref, smooth_sem):
    rows, basis = c_all.shape
    blocks = basis // LANES
    rank = test_ref.shape[0]
    halves = rows // LANES
    height = WINDOW
    base = rank + EDGE
    has_left = lax.axis_index("tm") > 0
    has_right = lax.axis_index("tm") < lax.axis_size("tm") - 1
    sub = lax.broadcasted_iota(jnp.int32, (8, LANES), 0)

    def tile_at(which):
        return pl.ds(pl.multiple_of(which * LANES, LANES), LANES)

    def incoming(which):
        at = pl.ds(pl.multiple_of(which * TILE, TILE), TILE)
        slot = lax.rem(which, DEPTH)
        return pltpu.make_async_copy(x_all.at[:, at], x_ref.at[slot], x_sems.at[slot])

    def outgoing(which):
        at = tile_at(which)
        return pltpu.make_async_copy(c_ref.at[:, at], c_all.at[:, at], c_sems.at[which])

    def project(step, between):
        slot = lax.rem(step, 2)

        def chunk_dot(r):
            high, low = split_bf16(x_ref[lax.rem(step, DEPTH), :, r * CHUNK : (r + 1) * CHUNK])
            w = w_ref[r * CHUNK : (r + 1) * CHUNK, :]
            return dot32(high, w) + dot32(low, w)

        count = TILE // CHUNK
        for _ in between:
            pass
        rest = chunk_dot(count - 1)
        last_ref[slot] = rest[:, :LANES] + rest[:, LANES:]
        most = None
        for r in range(count - 1):
            part = chunk_dot(r)
            most = part if most is None else most + part
        for _ in between:
            pass
        main_ref[slot] = most[:, :LANES] + most[:, LANES:]

    def relax(block, is_end=False):
        slot, before = lax.rem(block + 2, 2), lax.rem(block + 1, 2)
        is_first = block == 0
        write_at = jnp.maximum(block, 0) * LANES
        for h in range(halves):
            cols = slice(h * LANES, (h + 1) * LANES)
            proj_ref[h, 8:HEAD, :] = proj_ref[h, LANES + 8 : LANES + HEAD, :]
            wide = lax.broadcasted_iota(jnp.int32, (LANES, LANES), 1)
            earlier = jnp.where(is_first, 0.0, last_ref[before, cols, :])
            here = main_ref[slot, cols, :] + jnp.where(wide < LANES // 2, earlier, last_ref[slot, cols, :])
            turned = here.T
            proj_ref[h, HEAD : HEAD + LANES, :] = turned
            if not is_end:
                strip_ref[h] = jnp.where(is_first, turned[:EDGE], strip_ref[h])
            else:
                spilled = last_ref[slot, cols, :].T[:8]
                ending = jnp.concatenate([turned[LANES - ZONE_HIGH :], spilled], axis=0)
                strip_ref[h] = jnp.where(has_right, ending, strip_ref[h])

            smooth = jnp.broadcast_to(smooth_ref[:, cols], (8, LANES))
            starting = closing = inner = sweep_factors(smooth, 6.0)
            if not is_end:
                diag = jnp.where(sub == 0, 1.0, jnp.where(sub == 1, 5.0, 6.0))
                starting = sweep_factors(smooth, jnp.where(is_first, diag, 6.0))
            else:
                closing = sweep_factors(smooth, jnp.where(sub == 7, 1.0, jnp.where(sub == 6, 5.0, 6.0)))

            def ghosts(ref, lead):
                def row(at):
                    return jnp.broadcast_to(ref[(*lead, slice(at, at + 1), slice(None))], (8, LANES))

                if not is_end:
                    zero, one = row(HEAD), row(HEAD + 1)
                    ahead = (*lead, slice(HEAD - 8, HEAD), slice(None))
                    outside = jnp.where(sub == 7, 2.0 * zero - one, 3.0 * zero - 2.0 * one)
                    ref[ahead] = jnp.where(is_first, outside, ref[ahead])
                else:
                    zero, one = row(height - 1), row(height - 2)
                    ref[(*lead, slice(height, height + 8), slice(None))] = jnp.where(
                        sub == 0, 2.0 * zero - one, 3.0 * zero - 2.0 * one
                    )

            ghosts(proj_ref, (h,))
            source, lead = proj_ref, (h,)
            for sweep in range(ITERS):
                final = sweep == ITERS - 1

                def load(at):
                    return source[(*lead, slice(at, at + 8), slice(None))]

                values = []
                for at in range(16 if final else 8, height, 8):
                    value = relaxed(
                        load(at),
                        load(at - 1) + load(at + 1),
                        load(at - 2) + load(at + 2),
                        proj_ref[h, at : at + 8, :],
                        starting if at == HEAD else closing if at == height - 8 else inner,
                    )
                    if final:
                        done_ref[h, pl.ds(pl.multiple_of(write_at + at - 16, 8), 8), :] = value
                    else:
                        state_ref[sweep, h, at : at + 8, :] = value
                if not final:
                    ghosts(state_ref, (sweep, h))
                    source, lead = state_ref, (sweep, h)
                yield

    def finish(which, end=False):
        parts = []
        for h in range(halves):
            where = pl.multiple_of(which * LANES + 8, 8)
            part = done_ref[h, pl.ds(where, LANES), :]
            c_ref[h * LANES : (h + 1) * LANES, tile_at(which)] = part.T
            parts.append(part)
        test = test_ref[:, tile_at(which)]
        wide = lax.broadcasted_iota(jnp.int32, (rank, LANES), 1)
        if not end:
            left_zone = jnp.logical_and(has_left, which == 0)
            test = jnp.where(jnp.logical_and(left_zone, wide < ZONE_HIGH), 0.0, test)
        else:
            test = jnp.where(jnp.logical_and(has_right, wide >= LANES - ZONE_LOW), 0.0, test)
        test_high, test_low = split_bf16(test)
        high, low = split_bf16(jnp.concatenate(parts, axis=1))
        both = dot32(jnp.concatenate([test_high, test_low], axis=0), high)
        more = both[:rank] + both[rank:] + dot32(test_high, low)
        scored[...] = jnp.where(which == 0, 0.0, scored[...]) + more

    smooth_copy = pltpu.make_async_copy(smooth_all, smooth_ref, smooth_sem)
    test_copy = pltpu.make_async_copy(test_all, test_ref, test_sem)
    smooth_copy.start()
    for which in range(min(DEPTH - 1, blocks)):
        incoming(which).start()
    test_copy.start()
    band = banded_weights()
    for r in range(TILE // CHUNK):
        high, low = split_bf16(pltpu.roll(band, r * (CHUNK // SPB), 1))
        w_ref[r * CHUNK : (r + 1) * CHUNK, :LANES] = high
        w_ref[r * CHUNK : (r + 1) * CHUNK, LANES:] = low
    smooth_copy.wait()

    def advance(step):
        @pl.when(step + DEPTH - 1 < blocks)
        def _():
            incoming(step + DEPTH - 1).start()

        incoming(step).wait()

    @pl.loop(0, 3)
    def _(step):
        advance(step)
        project(step, relax(step - 1))

    test_copy.wait()

    @pl.loop(3, blocks)
    def _(step):
        advance(step)
        finish(step - 3)
        project(step, relax(step - 1))
        outgoing(step - 3).start()

    finish(blocks - 3)
    outgoing(blocks - 3).start()
    for _ in relax(blocks - 1, is_end=True):
        pass
    finish(blocks - 2)
    outgoing(blocks - 2).start()
    finish(blocks - 1, end=True)
    outgoing(blocks - 1).start()

    msg_ref[:rank, :] = scored[...]
    for h in range(halves):
        msg_ref[rank:base, h * LANES : (h + 1) * LANES] = strip_ref[h]
    low_zone = padded_turn(test_ref[:, basis - LANES :])[LANES - ZONE_LOW :]
    high_zone = padded_turn(test_ref[:, :LANES])
    msg_ref[base:, :] = jnp.zeros_like(msg_ref[base:, :])
    msg_ref[base:, :LANES] = jnp.where(has_right, low_zone, high_zone[:8])
    msg_ref[base:, LANES : 2 * LANES] = high_zone[8:16]
    for which in range(blocks):
        outgoing(which).wait()


def padded_turn(part):
    fill = jnp.zeros((LANES - part.shape[0], LANES), part.dtype)
    return jnp.concatenate([part, fill], axis=0).T


def curve_stage(samples, smooth_row, test_t):
    rows, width = samples.shape
    rank, basis = test_t.shape
    blocks, halves = basis // LANES, rows // LANES
    f32, bf16 = jnp.float32, jnp.bfloat16
    vmem, hbm = pl.BlockSpec(memory_space=pltpu.VMEM), pl.BlockSpec(memory_space=pltpu.HBM)
    return pl.pallas_call(
        curve_kernel,
        out_shape=(
            jax.ShapeDtypeStruct((rows, basis), f32),
            jax.ShapeDtypeStruct((rank + EDGE + 8, rows), f32),
        ),
        in_specs=[hbm, hbm, hbm],
        out_specs=(hbm, vmem),
        scratch_shapes=[
            pltpu.VMEM((TILE, 2 * LANES), bf16),
            pltpu.VMEM((2, rows, LANES), f32),
            pltpu.VMEM((2, rows, LANES), f32),
            pltpu.VMEM((halves, WINDOW + 8, LANES), f32),
            pltpu.VMEM((ITERS - 1, halves, WINDOW + 8, LANES), f32),
            pltpu.VMEM((halves, basis + LANES, LANES), f32),
            pltpu.VMEM((rank, rows), f32),
            pltpu.VMEM((halves, EDGE, LANES), f32),
            pltpu.VMEM((DEPTH, rows, TILE), f32),
            pltpu.SemaphoreType.DMA((DEPTH,)),
            pltpu.VMEM((rank, basis), f32),
            pltpu.SemaphoreType.DMA,
            pltpu.VMEM((rows, basis), f32),
            pltpu.SemaphoreType.DMA((blocks,)),
            pltpu.VMEM((1, rows), f32),
            pltpu.SemaphoreType.DMA,
        ],
        compiler_params=pltpu.CompilerParams(
            vmem_limit_bytes=60 * 1024 * 1024,
        ),
        cost_estimate=pl.CostEstimate(
            flops=4 * rows * width * 2 * LANES, bytes_accessed=4 * rows * width, transcendentals=0
        ),
        name="curves",
    )(samples, smooth_row, test_t)


def relax_strip(strip, smooth_row):
    factor = damping / (1.0 + 6.0 * smooth_row)
    pull = factor * smooth_row
    height = strip.shape[0]
    pulled = factor * strip
    state = strip

    def difference(v):
        return pltpu.roll(v, 1, 0) + pltpu.roll(v, height - 1, 0) - (v + v)

    for _ in range(ITERS):
        state = (1.0 - factor) * state + pulled - pull * difference(difference(state))
    return state


def swapped(value, block, flip):
    parts = [value[at : at + block] for at in range(0, value.shape[0], block)]
    other = [parts[k ^ 1] for k in range(len(parts))]
    return jnp.where(flip, jnp.concatenate(other, axis=0), value)


def exchange_order(value, order, index):
    count = 1 << len(order)
    block = value.shape[0] // count
    owner = [sum(b for k, b in enumerate(order) if p >> (len(order) - 1 - k) & 1) for p in range(count)]
    value = jnp.concatenate([value[q * block : (q + 1) * block] for q in owner], axis=0)
    for k, bit in enumerate(order):
        value = swapped(value, value.shape[0] >> (k + 1), (index & bit) != 0)
    return value


def sketch_kernel(order, own_ref, own_edge_ref, came_ref, smooth_ref, c_low, c_high, c_in, c_ref, keep_ref,
                  send_ref, total_ref, tile_ref, store_sem):
    rows, basis = c_in.shape
    wide = basis // 2
    rank = total_ref.shape[0]
    tiles = basis // LANES
    half = rank // 2
    has_left = lax.axis_index("tm") > 0
    own, came = own_ref[...], came_ref[:rank, :]
    own_edge, came_edge = own_edge_ref[...], came_ref[rank:, :]
    low = jnp.where(has_left, came_edge, own_edge)
    high = jnp.where(has_left, own_edge, came_edge)
    fill = jnp.zeros((EDGE - ZONE_LOW, rows), jnp.float32)
    strip = jnp.concatenate([low[:EDGE], fill], axis=0) + jnp.concatenate([fill, high[:EDGE]], axis=0)
    fixed = relax_strip(strip, smooth_ref[...])[ZONE_LOW : ZONE_LOW + EDGE]
    zone_test = jnp.concatenate(
        [low[EDGE:, :LANES], high[EDGE:, :LANES], high[EDGE:, LANES : 2 * LANES]], axis=0
    )[:, :rank]
    zone_scores = lax.dot_general(
        zone_test, fixed, (((0,), (0,)), ((), ())),
        precision=lax.Precision.HIGHEST, preferred_element_type=jnp.float32,
    )
    total = own + came + zone_scores
    total_ref[...] = total

    placed = jnp.where(
        has_left,
        jnp.concatenate([fixed[ZONE_LOW:], jnp.zeros((LANES - ZONE_HIGH, rows), jnp.float32)], axis=0),
        jnp.concatenate([jnp.zeros((LANES - ZONE_LOW, rows), jnp.float32), fixed[:ZONE_LOW]], axis=0),
    )
    lane = lax.broadcasted_iota(jnp.int32, (LANES, LANES), 1)
    first, past = jnp.where(has_left, 0, LANES - ZONE_LOW), jnp.where(has_left, ZONE_HIGH, LANES)
    fix_lane = jnp.logical_and(lane >= first, lane < past)
    edge = pl.multiple_of(jnp.where(has_left, 0, basis - LANES), LANES)

    mean_score = jnp.mean(total, axis=1, keepdims=True)
    spread = jnp.broadcast_to(mean_score, (rank, LANES))
    score_row = padded_turn(spread)[:8]
    index = lax.axis_index("curve")
    spread = exchange_order(spread, order, index)
    lhs_high, lhs_low = split_bf16(exchange_order(total - mean_score, order, index))
    lhs = jnp.concatenate([lhs_high, lhs_low], axis=0)

    placed = [placed[:, at : at + LANES].T for at in range(0, rows, LANES)]
    placed = jnp.concatenate(placed, axis=0)
    fix_lane = jnp.concatenate([fix_lane.astype(jnp.int32)] * (rows // LANES), axis=0)
    store = pltpu.make_async_copy(tile_ref, c_ref.at[:, pl.ds(edge, LANES)], store_sem)

    for b in range(tiles):
        part, at = (c_low, b * LANES) if b * LANES < wide else (c_high, b * LANES - wide)
        block = part[:, at : at + LANES]
        if b in (0, tiles - 1):
            mine = has_left if b == 0 else jnp.logical_not(has_left)
            block = jnp.where(fix_lane * mine.astype(jnp.int32) > 0, placed, block)
            tile_ref[...] = block if b == 0 else jnp.where(has_left, tile_ref[...], block)
        mean = jnp.mean(block, axis=0, keepdims=True)
        rhs_high, rhs_low = split_bf16(block - mean)
        out = dot32(lhs, rhs_high)
        out = out[:rank] + out[rank:] + dot32(lhs_high, rhs_low)
        keep_ref[b * half : (b + 1) * half, :] = out[:half]
        send_ref[b * half : (b + 1) * half, :] = out[half:]
        at = (tiles + 1) * half + b
        keep_ref[at : at + 1, :] = mean
        send_ref[at : at + 1, :] = mean
    store.start()
    at = tiles * half
    keep_ref[at : at + half, :] = spread[:half]
    send_ref[at : at + half, :] = spread[half:]
    at = (tiles + 1) * half + tiles
    keep_ref[at:, :] = score_row
    send_ref[at:, :] = score_row
    store.wait()


def sketch_stage(message, came, smooth_row, coefficients, rank, order):
    rows, basis = coefficients.shape
    tiles = basis // LANES
    half = rank // 2
    f32 = jnp.float32
    packed = jax.ShapeDtypeStruct(((tiles + 1) * half + tiles + 8, LANES), f32)
    vmem, hbm = pl.BlockSpec(memory_space=pltpu.VMEM), pl.BlockSpec(memory_space=pltpu.HBM)
    return pl.pallas_call(
        functools.partial(sketch_kernel, order),
        out_shape=(
            jax.ShapeDtypeStruct((rows, basis), f32), packed, packed,
            jax.ShapeDtypeStruct((rank, rows), f32),
        ),
        in_specs=[vmem] * 6 + [hbm],
        out_specs=(hbm, vmem, vmem, vmem),
        scratch_shapes=[
            pltpu.VMEM((rows, LANES), f32),
            pltpu.SemaphoreType.DMA,
        ],
        input_output_aliases={6: 0},
        compiler_params=pltpu.CompilerParams(vmem_limit_bytes=16 * 1024 * 1024),
        cost_estimate=pl.CostEstimate(
            flops=6 * rows * basis * rank, bytes_accessed=4 * rows * basis, transcendentals=0
        ),
        name="sketch_part",
    )(
        message[:rank], message[rank:], came, smooth_row,
        coefficients[:, : basis // 2], coefficients[:, basis // 2 :], coefficients,
    )


def unpack(packed, tiles, height):
    moment = packed[: tiles * height].reshape(tiles, height, LANES)
    score = packed[tiles * height : (tiles + 1) * height]
    rest = packed[(tiles + 1) * height :]
    return moment, score, rest


def merged(one, other, count):
    moment, score, rest = one
    moment_2, score_2, rest_2 = other
    tiles = moment.shape[0]
    apart = rest[:tiles] - rest_2[:tiles]
    moment = moment + moment_2 + (0.5 * count) * apart[:, None, :] * (score - score_2)[None]
    return moment, 0.5 * (score + score_2), 0.5 * (rest + rest_2)


def packed_share(group, which, shares):
    moment, score, rest = group
    height = moment.shape[1] // shares
    part = slice(which * height, (which + 1) * height)
    return jnp.concatenate([moment[:, part].reshape(-1, LANES), score[part], rest], axis=0)


def exchanged(packed, groups, bits):
    return lax.ppermute(packed, "curve", [(i, i ^ bits) for i in range(groups)])


def fast_body(samples, smoothing, test_matrix, sketch_prev):
    rows, basis = samples.shape[0], test_matrix.shape[0]
    rank = test_matrix.shape[1]
    tiles = basis // LANES
    groups = lax.axis_size("curve")
    order = [1 << k for k in range(groups.bit_length() - 1)]
    smooth_row = smoothing[None, :]
    coefficients, message = curve_stage(samples, smooth_row, test_matrix.T)
    came = lax.ppermute(message, "tm", [(0, 1), (1, 0)])
    coefficients, keep, send, total = sketch_stage(message, came, smooth_row, coefficients, rank, order)
    height, count = rank // 2, rows
    came = exchanged(send, groups, order[0])
    group = merged(unpack(keep, tiles, height), unpack(came, tiles, height), count)
    count *= 2
    rest = order[1:]
    while rest:
        bits, rest = rest[:RADIX_BITS], rest[RADIX_BITS:]
        shares = 1 << len(bits)
        height //= shares
        parts = [unpack(packed_share(group, 0, shares), tiles, height)]
        for which in range(1, shares):
            partner = sum(b for k, b in enumerate(bits) if which >> (len(bits) - 1 - k) & 1)
            came = exchanged(packed_share(group, which, shares), groups, partner)
            parts.append(unpack(came, tiles, height))
        while len(parts) > 1:
            parts = [merged(parts[k], parts[k + 1], count) for k in range(0, len(parts), 2)]
            count *= 2
        group = parts[0]
    moment, _, rest = group
    score_mean = rest[tiles, :rank]
    scores = (total - score_mean[:, None]).T
    sketch = sketch_prev + moment.transpose(0, 2, 1).reshape(basis, height) / count
    return coefficients, scores, sketch


def passed_along(block, axis, distance):
    devices = range(lax.axis_size(axis))
    route = [(i - distance, i) for i in devices if i - distance in devices]
    return lax.ppermute(block, axis, route)


def padded_2(block, sides, width):
    for axis, dim in sides:
        count = lax.axis_size(axis)
        forward = [(i, i + 1) for i in range(count - 1)]
        backward = [(target, source) for source, target in forward]
        low = lax.ppermute(
            lax.slice_in_dim(block, block.shape[dim] - width, None, axis=dim), axis, forward
        )
        high = lax.ppermute(lax.slice_in_dim(block, 0, width, axis=dim), axis, backward)
        block = jnp.concatenate([low, block, high], axis=dim)
    return block


def weight_table():
    frac = (jnp.arange(SPB, dtype=jnp.float32) + 0.5) / SPB
    pieces = [
        frac**3 / 6.0,
        (-3.0 * frac**3 + 3.0 * frac**2 + 3.0 * frac + 1.0) / 6.0,
        (3.0 * frac**3 - 6.0 * frac**2 + 4.0) / 6.0,
        (1.0 - frac) ** 3 / 6.0,
    ]
    return jnp.stack(pieces) / SPB


def relax_sweep(widened, target, smooth_col, index_wide, total_basis):
    second = widened[:, 2:] - 2.0 * widened[:, 1:-1] + widened[:, :-2]
    in_range = (index_wide[:-2] >= 0) & (index_wide[:-2] <= total_basis - 3)
    second = jnp.where(in_range[None, :], second, 0.0)
    bending = second[:, 2:] - 2.0 * second[:, 1:-1] + second[:, :-2]
    interior = widened[:, 2:-2]
    column_index = index_wide[2:-2]
    penalty_diag = (
        (column_index <= total_basis - 3).astype(jnp.float32)
        + 4.0 * ((column_index >= 1) & (column_index <= total_basis - 2)).astype(jnp.float32)
        + (column_index >= 2).astype(jnp.float32)
    )
    return interior + damping * (target - interior - smooth_col * bending) / (
        1.0 + smooth_col * penalty_diag
    )


def plain_body(samples, smoothing, test_matrix, sketch_prev):
    row_count = samples.shape[0]
    basis_width = samples.shape[1] // SPB
    blocks = samples.reshape(row_count, basis_width, SPB)
    segment_sums = jnp.einsum(
        "cgq,mq->mcg", blocks, weight_table(), precision=lax.Precision.HIGHEST
    )
    padded = jnp.pad(segment_sums, ((0, 0), (0, 0), (3, 3)))
    extended = (
        padded[0, :, 0 : basis_width + 3]
        + padded[1, :, 1 : basis_width + 4]
        + padded[2, :, 2 : basis_width + 5]
        + padded[3, :, 3 : basis_width + 6]
    )
    spilled = extended[:, basis_width:]
    arrived = passed_along(spilled, "tm", 1)
    proj = jnp.concatenate([extended[:, :3] + arrived, extended[:, 3:basis_width]], axis=1)
    total_basis = basis_width * lax.axis_size("tm")
    first_column = lax.axis_index("tm") * basis_width
    smooth_col = smoothing[:, None]
    margin = 2 * ITERS
    proj_wide = padded_2(proj, (("tm", 1),), margin)
    coefficients = proj_wide
    for sweep_number in range(ITERS):
        margin_now = margin - 2 * sweep_number
        index_wide = (
            first_column - margin_now + jnp.arange(basis_width + 2 * margin_now, dtype=jnp.int32)
        )
        offset = 2 * sweep_number + 2
        target = proj_wide[:, offset : offset + basis_width + 2 * margin_now - 4]
        coefficients = relax_sweep(coefficients, target, smooth_col, index_wide, total_basis)
    curve_total = row_count * lax.axis_size("curve")
    totals = lax.psum(jnp.sum(coefficients, axis=0), "curve")
    column_mean = totals / curve_total
    centered = coefficients - column_mean[None, :]
    partial_value = jnp.dot(
        centered, test_matrix, precision=lax.Precision.HIGHEST, preferred_element_type=jnp.float32
    )
    scores = lax.psum(partial_value, "tm")
    sketch_part = (
        jnp.einsum("ck,cr->kr", centered, scores, precision=lax.Precision.HIGHEST) / curve_total
    )
    owned_part = lax.psum_scatter(sketch_part, "curve", scatter_dimension=1, tiled=True)
    return (coefficients, scores, sketch_prev + owned_part)


def fits(mesh):
    groups = mesh.shape["curve"]
    return mesh.shape["tm"] == 2 and groups > 1 and groups & (groups - 1) == 0


def solution(mesh):
    placed = (P("curve", "tm"), P("curve"), P("tm", None), P("tm", "curve"))
    return jax.shard_map(
        fast_body if fits(mesh) else plain_body,
        mesh=mesh,
        in_specs=placed,
        out_specs=(P("curve", "tm"), P("curve", None), P("tm", "curve")),
        check_vma=False,
    )
```
